32 devices in a mesh: dp: 1 (over z), tp: 32 (over y, x, core).
Axes of the slice: x: 4, y: 4, z: 1, core: 2. Of those that a mesh axis runs over, the one named last changes fastest.
The devices are a block of a 4x4x8 slice.
Arguments:
- x_in: bfloat16 [1, 4096, 2048], P('dp', 'tp')
- ln1_gain: float32 [2, 2048], replicated
- w_qkv: bfloat16 [2, 2048, 32, 192], P(None, None, 'tp')
- w_out: bfloat16 [2, 32, 64, 2048], P(None, 'tp')
- ln2_gain: float32 [2, 2048], replicated
- w_up: bfloat16 [2, 2048, 8192], P(None, None, 'tp')
- w_down: bfloat16 [2, 8192, 2048], P(None, 'tp')
Outputs:
- output: bfloat16 [1, 4096, 2048], P('dp', 'tp')
All inputs are finite; a program needn't handle non-finite values.
Results may differ from the reference program's by a relative error of at most 0.02.
Values are sent between devices in bfloat16 or wider.
A program may use at most 768 MiB of HBM per device.

```python
import jax
import jax.numpy as jnp
from jax import lax

D = 2048
HEADS = 32
FF = 8192
LAYERS = 2
BATCH = 1
SEQ = 4096
HEAD_DIM = D // HEADS
LN_EPS = 1.0e-5
NEG_BIG = -1.0e30


def setup_inputs(seed: int = 0, part: int = 0) -> dict:
    base_key = jax.random.key(seed)
    key_list = jax.random.split(base_key, 7)
    x_in = jax.random.normal(jax.random.fold_in(key_list[0], part), (BATCH, SEQ, D), jnp.float32)
    ln1_gain = jax.random.uniform(key_list[1], (LAYERS, D), jnp.float32, 1.2, 2.0)
    w_qkv = jax.random.normal(key_list[2], (LAYERS, D, HEADS, 3 * HEAD_DIM), jnp.float32) * D ** -0.5
    w_out = jax.random.normal(key_list[3], (LAYERS, HEADS, HEAD_DIM, D), jnp.float32) * D ** -0.5
    ln2_gain = jax.random.uniform(key_list[4], (LAYERS, D), jnp.float32, 0.7, 1.5)
    w_up = jax.random.normal(key_list[5], (LAYERS, D, FF), jnp.float32) * D ** -0.5
    w_down = jax.random.normal(key_list[6], (LAYERS, FF, D), jnp.float32) * FF ** -0.5
    return {'x_in': x_in.astype(jnp.bfloat16), 'ln1_gain': ln1_gain, 'w_qkv': w_qkv.astype(jnp.bfloat16), 'w_out': w_out.astype(jnp.bfloat16), 'ln2_gain': ln2_gain, 'w_up': w_up.astype(jnp.bfloat16), 'w_down': w_down.astype(jnp.bfloat16)}


def layer_norm(residual, ln_gain):
    resid_f32 = residual.astype(jnp.float32)
    row_mean = jnp.mean(resid_f32, axis=-1, keepdims=True)
    centered = resid_f32 - row_mean
    row_var = jnp.mean(centered * centered, axis=-1, keepdims=True)
    return (centered * lax.rsqrt(row_var + LN_EPS) * ln_gain).astype(jnp.bfloat16)


def attend_head(qkv_head):
    query_blk = qkv_head[:, :HEAD_DIM]
    key_blk = qkv_head[:, HEAD_DIM:2 * HEAD_DIM]
    value_blk = qkv_head[:, 2 * HEAD_DIM:]
    scores = jnp.dot(query_blk, key_blk.T, preferred_element_type=jnp.float32) * HEAD_DIM ** -0.5
    positions = jnp.arange(SEQ)
    scores = jnp.where(positions[:, None] >= positions[None, :], scores, NEG_BIG)
    attn_probs = jax.nn.softmax(scores, axis=-1).astype(jnp.bfloat16)
    return jnp.dot(attn_probs, value_blk, preferred_element_type=jnp.float32).astype(jnp.bfloat16)


def reference(x_in, ln1_gain, w_qkv, w_out, ln2_gain, w_up, w_down):
    def one_layer(residual, layer_weights):
        gain_one, qkv_weight, out_weight, gain_two, up_weight, down_weight = layer_weights
        normed = layer_norm(residual, gain_one)
        qkv_all = jnp.dot(normed, qkv_weight.reshape(D, 3 * D), preferred_element_type=jnp.float32).astype(jnp.bfloat16)
        qkv_heads = qkv_all.reshape(BATCH, SEQ, HEADS, 3 * HEAD_DIM).transpose(0, 2, 1, 3).reshape(BATCH * HEADS, SEQ, 3 * HEAD_DIM)
        attended = lax.map(attend_head, qkv_heads)
        attended = attended.reshape(BATCH, HEADS, SEQ, HEAD_DIM).transpose(0, 2, 1, 3).reshape(BATCH * SEQ, D)
        attn_proj = jnp.dot(attended, out_weight.reshape(D, D), preferred_element_type=jnp.float32)
        residual = (residual.astype(jnp.float32) + attn_proj).astype(jnp.bfloat16)
        normed = layer_norm(residual, gain_two)
        hidden = jax.nn.gelu(jnp.dot(normed, up_weight, preferred_element_type=jnp.float32), approximate=True).astype(jnp.bfloat16)
        down_out = jnp.dot(hidden, down_weight, preferred_element_type=jnp.float32)
        residual = (residual.astype(jnp.float32) + down_out).astype(jnp.bfloat16)
        return residual, None
    resid_out, _ = lax.scan(one_layer, x_in.reshape(BATCH * SEQ, D), (ln1_gain, w_qkv, w_out, ln2_gain, w_up, w_down))
    return resid_out.reshape(BATCH, SEQ, D)
```

```python
import functools
import math

import jax
import jax.numpy as jnp
from jax import lax
from jax.experimental import pallas as pl
from jax.experimental.pallas import tpu as pltpu
from jax.sharding import PartitionSpec as P

LN_EPS = 1.0e-5
NEG_BIG = -1.0e30
MESH = pl.DeviceIdType.MESH
CORES = 2
VMEM_LIMIT = 67043328
OWN, LEFT, RIGHT, OPP = 0, 1, 2, 3
RING = 4


def layer_norm(resid_f32, ln_gain):
    row_mean = jnp.mean(resid_f32, axis=-1, keepdims=True)
    centered = resid_f32 - row_mean
    row_var = jnp.mean(centered * centered, axis=-1, keepdims=True)
    return (centered * lax.rsqrt(row_var + LN_EPS) * ln_gain).astype(jnp.bfloat16)


def dot(a, b, dims=((1,), (0,))):
    return lax.dot_general(a, b, (dims, ((), ())), preferred_element_type=jnp.float32)


class Ids:
    def __init__(self):
        self.count = 0

    def take(self, n):
        first = self.count
        self.count += n
        return first


def stack_kernel(layers, x_ref, g1_ref, g2_ref, wqt_ref, wo_ref, wu_ref, wd_ref, out_ref,
                 xg_a, xg_m, wq, wot, wu, wd, stage, qkv, keys, vals, ostage, osum, oall,
                 acc, own, psend, precv, hop, comb, direct, hid, res,
                 send_sem, recv_sem, local_sem, ids):
    rows, width = res.shape
    half = rows // 2
    me = lax.axis_index("tp")
    core = lax.rem(me, CORES)
    other = 1 - core
    xpos = lax.rem(lax.div(me, CORES), RING)
    ypos = lax.div(me, CORES * RING)

    def dev(y, x, c):
        return (lax.rem(y, RING) * RING + lax.rem(x, RING)) * CORES + c

    partner = dev(ypos, xpos, other)
    xdev = {LEFT: dev(ypos, xpos + 3, core), RIGHT: dev(ypos, xpos + 1, core), OPP: dev(ypos, xpos + 2, core)}
    ydev = {LEFT: dev(ypos + 3, xpos, core), RIGHT: dev(ypos + 1, xpos, core)}

    pending, pending_weights = [], []

    def send(k, src, dst, device, queue=pending):
        copy = pltpu.make_async_remote_copy(src_ref=src, dst_ref=dst, send_sem=send_sem.at[k], recv_sem=recv_sem.at[k],
                                            device_id={"tp": device}, device_id_type=MESH)
        copy.start()
        queue.append(copy)

    def arrived(k, dst):
        pltpu.make_async_remote_copy(src_ref=dst, dst_ref=dst, send_sem=send_sem.at[k], recv_sem=recv_sem.at[k],
                                     device_id={"tp": partner}, device_id_type=MESH).wait_recv()

    def drain(queue=pending):
        for copy in queue:
            copy.wait_send()
        queue.clear()

    class Gather:
        def __init__(self, buf, ring):
            self.buf, self.ring, self.k = buf, ring, ids.take(12)
            self.a, self.b = pl.ds(0, half), pl.ds(half, half)

        def start(self):
            own_rows = self.buf.at[OWN, core]
            right, left = self.ring[RIGHT], self.ring[LEFT]
            send(self.k, own_rows.at[self.a], self.buf.at[LEFT, core, self.a], right)
            send(self.k + 1, own_rows.at[self.b], self.buf.at[RIGHT, core, self.b], left)
            send(self.k + 2, own_rows, self.buf.at[OWN, core], partner)
            send(self.k + 3, own_rows.at[self.b], self.buf.at[LEFT, core, self.b], right)
            send(self.k + 4, own_rows.at[self.a], self.buf.at[RIGHT, core, self.a], left)

        def relay(self):
            arrived(self.k, self.buf.at[LEFT, core, self.a])
            send(self.k + 5, self.buf.at[LEFT, core, self.a], self.buf.at[OPP, core, self.a], self.ring[RIGHT])
            arrived(self.k + 1, self.buf.at[RIGHT, core, self.b])
            send(self.k + 6, self.buf.at[RIGHT, core, self.b], self.buf.at[OPP, core, self.b], self.ring[LEFT])

        def near(self):
            arrived(self.k + 3, self.buf.at[LEFT, core, self.b])
            send(self.k + 7, self.buf.at[LEFT, core], self.buf.at[LEFT, core], partner)
            arrived(self.k + 4, self.buf.at[RIGHT, core, self.a])
            send(self.k + 8, self.buf.at[RIGHT, core], self.buf.at[RIGHT, core], partner)

        def far(self):
            arrived(self.k + 5, self.buf.at[OPP, core, self.a])
            arrived(self.k + 6, self.buf.at[OPP, core, self.b])
            send(self.k + 9, self.buf.at[OPP, core], self.buf.at[OPP, core], partner)

        def wait(self, slot):
            arrived(self.k + {OWN: 2, LEFT: 7, RIGHT: 8, OPP: 9}[slot], self.buf.at[slot, other])

    class Weights:
        def __init__(self, src, buf, ring):
            self.src, self.buf, self.ring = src, buf, ring
            self.k = ids.take(6)
            n = buf.shape[1] // 2
            self.a, self.b = pl.ds(0, n), pl.ds(n, n)

        def local(self, sem):
            copy = pltpu.make_async_copy(self.src, self.buf.at[OWN], local_sem.at[sem])
            copy.start()
            return copy

        def start(self):
            right, left = self.ring[RIGHT], self.ring[LEFT]
            send(self.k, self.src.at[self.a], self.buf.at[LEFT, self.a], right, pending_weights)
            send(self.k + 1, self.src.at[self.b], self.buf.at[RIGHT, self.b], left, pending_weights)
            send(self.k + 2, self.src.at[self.b], self.buf.at[LEFT, self.b], right, pending_weights)
            send(self.k + 3, self.src.at[self.a], self.buf.at[RIGHT, self.a], left, pending_weights)

        def relay(self):
            arrived(self.k, self.buf.at[LEFT, self.a])
            send(self.k + 4, self.buf.at[LEFT, self.a], self.buf.at[OPP, self.a], self.ring[RIGHT], pending_weights)
            arrived(self.k + 1, self.buf.at[RIGHT, self.b])
            send(self.k + 5, self.buf.at[RIGHT, self.b], self.buf.at[OPP, self.b], self.ring[LEFT], pending_weights)

        def wait_near(self):
            arrived(self.k + 2, self.buf.at[LEFT, self.b])
            arrived(self.k + 3, self.buf.at[RIGHT, self.a])

        def wait_far(self):
            arrived(self.k + 4, self.buf.at[OPP, self.a])
            arrived(self.k + 5, self.buf.at[OPP, self.b])

    class Reduce:
        def __init__(self, ring):
            self.ring, self.k = ring, ids.take(10)
            self.a, self.b = pl.ds(0, half), pl.ds(half, half)

        def give(self, slot):
            own[slot] = acc[core]
            psend[slot] = acc[other].astype(jnp.bfloat16)
            send(self.k + slot, psend.at[slot], precv.at[slot], partner)

        def pair(self, slot):
            arrived(self.k + slot, precv.at[slot])

        def term(self, slot, part):
            return own[slot, part, :] + precv[slot, part, :].astype(jnp.float32)

        def far(self):
            self.pair(OPP)
            comb[0] = self.term(OPP, self.a).astype(jnp.bfloat16)
            send(self.k + 4, comb.at[0], hop.at[0], self.ring[RIGHT])
            comb[1] = self.term(OPP, self.b).astype(jnp.bfloat16)
            send(self.k + 5, comb.at[1], hop.at[1], self.ring[LEFT])

        def near(self, slot):
            self.pair(slot)
            if slot == RIGHT:
                comb[2] = self.term(RIGHT, self.b).astype(jnp.bfloat16)
                send(self.k + 6, comb.at[2], direct.at[0, 1], self.ring[RIGHT])
            else:
                comb[3] = self.term(LEFT, self.a).astype(jnp.bfloat16)
                send(self.k + 7, comb.at[3], direct.at[1, 0], self.ring[LEFT])

        def relay(self):
            arrived(self.k + 4, hop.at[0])
            comb[4] = (self.term(RIGHT, self.a) + hop[0].astype(jnp.float32)).astype(jnp.bfloat16)
            send(self.k + 8, comb.at[4], direct.at[0, 0], self.ring[RIGHT])
            arrived(self.k + 5, hop.at[1])
            comb[5] = (self.term(LEFT, self.b) + hop[1].astype(jnp.float32)).astype(jnp.bfloat16)
            send(self.k + 9, comb.at[5], direct.at[1, 1], self.ring[LEFT])

        def finish(self):
            self.pair(OWN)
            arrived(self.k + 6, direct.at[0, 1])
            arrived(self.k + 7, direct.at[1, 0])
            arrived(self.k + 8, direct.at[0, 0])
            arrived(self.k + 9, direct.at[1, 1])
            for i, part in enumerate((self.a, self.b)):
                total = self.term(OWN, part) + direct[0, i].astype(jnp.float32) + direct[1, i].astype(jnp.float32)
                res[part, :] = (res[part, :].astype(jnp.float32) + total).astype(jnp.bfloat16)

    w_q = [Weights(wqt_ref.at[l], wq.at[l], xdev) for l in range(layers)]
    w_o = [Weights(wo_ref.at[l], wot.at[l], xdev) for l in range(layers)]
    w_u = [Weights(wu_ref.at[l], wu.at[l], ydev) for l in range(layers)]
    w_d = [Weights(wd_ref.at[l], wd.at[l], ydev) for l in range(layers)]
    everything = [w for l in range(layers) for w in (w_q[l], w_o[l], w_u[l], w_d[l])]
    copies = [w.local(i) for i, w in enumerate(everything)]

    barrier = pltpu.get_barrier_semaphore()
    peers = [partner, *xdev.values(), *ydev.values()]
    for peer in peers:
        pl.semaphore_signal(barrier, inc=1, device_id={"tp": peer}, device_id_type=MESH)
    res[...] = x_ref[...]
    pl.semaphore_wait(barrier, len(peers))

    head_dim = keys.shape[1]
    block = qkv.shape[2]
    column = RING * block

    def attention_front(l, gather):
        k = ids.take(3 * RING)
        slots = {LEFT: RIGHT, RIGHT: LEFT, OPP: OPP}
        order = (OWN, LEFT, RIGHT, OPP)

        def heads(s, slot):
            rows_in = xg_a[s].reshape(CORES * rows, width)
            part = dot(wq[l, slot], rows_in, ((1,), (1,))).astype(jnp.bfloat16)
            shift = {OWN: 0, LEFT: 3, RIGHT: 1, OPP: 2}[s]
            g = lax.rem(ypos + shift, RING) * RING + xpos
            if slot == OWN:
                qkv[g] = part
            else:
                stage[s, slot - 1] = part
                send(k + 3 * s + slot - 1, stage.at[s, slot - 1], qkv.at[g], xdev[slot])

        def receive():
            for s in order:
                shift = {OWN: 0, LEFT: 3, RIGHT: 1, OPP: 2}[s]
                for slot in (LEFT, RIGHT, OPP):
                    x_from = {LEFT: xpos + 1, RIGHT: xpos + 3, OPP: xpos + 2}[slot]
                    g = lax.rem(ypos + shift, RING) * RING + lax.rem(x_from, RING)
                    arrived(k + 3 * s + slot - 1, qkv.at[g])

        return heads, receive

    def prepare_keys():
        def body(g, carry):
            keys[pl.ds(pl.multiple_of(g * block, block), block), :] = (
                qkv[g, head_dim:2 * head_dim, :].astype(jnp.float32).T.astype(jnp.bfloat16))
            vals[g // RING, :, pl.ds(pl.multiple_of(lax.rem(g, RING) * block, block), block)] = qkv[g, 2 * head_dim:, :]
            return carry

        lax.fori_loop(0, RING * RING, body, 0)

    def attend(shift):
        y = lax.rem(ypos + shift, RING)

        def one_block(x, carry):
            g = y * RING + x
            query = (qkv[g, :head_dim, :].astype(jnp.float32) * head_dim ** -0.5).astype(jnp.bfloat16)

            def scores(chunk):
                return dot(keys[pl.ds(pl.multiple_of(chunk * column, column), column), :], query)

            s = scores(y)
            key_pos = lax.broadcasted_iota(jnp.int32, s.shape, 0)
            query_pos = lax.broadcasted_iota(jnp.int32, s.shape, 1) + x * block
            s = jnp.where(query_pos >= key_pos, s, NEG_BIG)
            top = jnp.max(s, axis=0, keepdims=True)
            p = jnp.exp(s - top)
            total = jnp.sum(p, axis=0, keepdims=True)
            osum[...] = dot(vals[y], p.astype(jnp.bfloat16))

            def more(chunk, state):
                top, total = state
                s = scores(chunk)
                new_top = jnp.maximum(top, jnp.max(s, axis=0, keepdims=True))
                scale = jnp.exp(top - new_top)
                p = jnp.exp(s - new_top)
                total = total * scale + jnp.sum(p, axis=0, keepdims=True)
                osum[...] = osum[...] * scale + dot(vals[chunk], p.astype(jnp.bfloat16))
                return new_top, total

            top, total = lax.fori_loop(0, y, more, (top, total))
            ostage[shift, x] = (osum[...] / total).astype(jnp.bfloat16)
            return carry

        lax.fori_loop(0, RING, one_block, 0)

    def exchange_o(shift, k):
        oall[shift, OWN] = ostage[shift, xpos]
        for slot, x_to in ((LEFT, xpos + 1), (RIGHT, xpos + 3), (OPP, xpos + 2)):
            to = {LEFT: xdev[RIGHT], RIGHT: xdev[LEFT], OPP: xdev[OPP]}[slot]
            send(k + slot - 1, ostage.at[shift, lax.rem(x_to, RING)], oall.at[shift, slot], to)

    def project(l, shift, slot, k, reduce):
        for source in (LEFT, RIGHT, OPP):
            arrived(k + source - 1, oall.at[shift, source])
        o_all = oall[shift].reshape(RING * head_dim, block)
        w_all = wot[l].reshape(RING * head_dim, width)
        acc[...] = dot(o_all, w_all, ((0,), (0,))).reshape(acc.shape)
        reduce.give(slot)

    def mlp_slot(l, s, reduce):
        def up(j, carry):
            rows_in = xg_m[s].reshape(CORES * rows, width)
            h = jax.nn.gelu(dot(rows_in, wu[l, j]), approximate=True).astype(jnp.bfloat16)
            hid[:, pl.ds(pl.multiple_of(j * wu.shape[3], wu.shape[3]), wu.shape[3])] = h
            return carry

        lax.fori_loop(0, RING, up, 0)
        tile = 512

        def down(j, carry):
            cols = pl.ds(pl.multiple_of(j * tile, tile), tile)
            w_all = wd[l, :, :, cols].reshape(hid.shape[1], tile)
            acc[:, :, cols] = dot(hid[...], w_all).reshape(CORES, rows, tile)
            return carry

        lax.fori_loop(0, width // tile, down, 0)
        reduce.give(s)

    for l in range(layers):
        drain()
        gather = Gather(xg_a, ydev)
        xg_a[OWN, core] = layer_norm(res[...].astype(jnp.float32), g1_ref[l, :][None, :])
        gather.start()
        if l == 0:
            w_q[0].start()
            w_o[0].start()
        gather.relay()
        gather.near()
        if l == 0:
            w_q[0].relay()
            w_o[0].relay()
        gather.far()
        if l == 0:
            w_u[0].start()
            w_d[0].start()
            for i in range(2):
                copies[i].wait()
        w_q[l].wait_near()
        heads, receive = attention_front(l, gather)
        for s in (OWN, LEFT, RIGHT, OPP):
            gather.wait(s)
            if s == OWN:
                w_q[l].wait_far()
            for slot in (LEFT, RIGHT, OPP, OWN):
                heads(s, slot)
        if l == 0:
            w_u[0].relay()
        receive()
        prepare_keys()
        if l + 1 < layers:
            w_q[l + 1].start()
            w_o[l + 1].start()
        k_o = ids.take(3 * RING)
        reduce = Reduce(ydev)
        order = ((2, OPP), (3, LEFT), (1, RIGHT), (0, OWN))

        def finish_segment(i):
            shift, slot = order[i]
            project(l, shift, slot, k_o + 3 * shift, reduce)

        w_o[l].wait_near()
        w_o[l].wait_far()
        for i, (shift, slot) in enumerate(order):
            attend(shift)
            exchange_o(shift, k_o + 3 * shift)
            if i == 1:
                finish_segment(0)
            if i == 2:
                reduce.far()
                finish_segment(1)
                if l == 0:
                    w_d[0].relay()
                if l + 1 < layers:
                    w_q[l + 1].relay()
            if i == 3:
                reduce.near(LEFT)
                finish_segment(2)
        reduce.near(RIGHT)
        finish_segment(3)
        reduce.relay()
        reduce.finish()
        if l + 1 < layers:
            w_o[l + 1].relay()
        drain()

        gather = Gather(xg_m, xdev)
        xg_m[OWN, core] = layer_norm(res[...].astype(jnp.float32), g2_ref[l, :][None, :])
        gather.start()
        if l + 1 < layers:
            w_u[l + 1].start()
            w_d[l + 1].start()
        if l == 0:
            for i in range(2, len(copies)):
                copies[i].wait()
        reduce = Reduce(xdev)
        gather.relay()
        w_u[l].wait_near()
        w_d[l].wait_near()
        w_u[l].wait_far()
        w_d[l].wait_far()
        gather.wait(OWN)
        mlp_slot(l, OWN, reduce)
        gather.near()
        gather.wait(LEFT)
        mlp_slot(l, LEFT, reduce)
        reduce.near(LEFT)
        gather.far()
        gather.wait(RIGHT)
        mlp_slot(l, RIGHT, reduce)
        reduce.near(RIGHT)
        gather.wait(OPP)
        mlp_slot(l, OPP, reduce)
        reduce.far()
        if l + 1 < layers:
            w_u[l + 1].relay()
        reduce.relay()
        if l + 1 < layers:
            w_d[l + 1].relay()
        reduce.finish()
    drain()
    drain(pending_weights)
    out_ref[...] = res[...]


def solution(mesh):
    def layer_stack(x_local, ln1_gain, w_qkv, w_out, ln2_gain, w_up, w_down):
        batch, rows, width = x_local.shape
        layers, _, _, three_e = w_qkv.shape
        head_dim = three_e // 3
        ff = w_up.shape[2]
        block = CORES * rows
        wqt = w_qkv.reshape(layers, width, three_e).transpose(0, 2, 1)
        wo = w_out.reshape(layers, head_dim, width)
        bf16, f32 = jnp.bfloat16, jnp.float32
        vmem = pltpu.VMEM
        n_ids = 200
        hbm = pl.BlockSpec(memory_space=pltpu.HBM)
        in_vmem = pl.BlockSpec(memory_space=pltpu.VMEM)
        scratch = [
            vmem((RING, CORES, rows, width), bf16),
            vmem((RING, CORES, rows, width), bf16),
            vmem((layers, RING, three_e, width), bf16),
            vmem((layers, RING, head_dim, width), bf16),
            vmem((layers, RING, width, ff), bf16),
            vmem((layers, RING, ff, width), bf16),
            vmem((RING, RING - 1, three_e, block), bf16),
            vmem((RING * RING, three_e, block), bf16),
            vmem((RING * RING * block, head_dim), bf16),
            vmem((RING, head_dim, RING * block), bf16),
            vmem((RING, RING, head_dim, block), bf16),
            vmem((head_dim, block), f32),
            vmem((RING, RING, head_dim, block), bf16),
            vmem((CORES, rows, width), f32),
            vmem((RING, rows, width), f32),
            vmem((RING, rows, width), bf16),
            vmem((RING, rows, width), bf16),
            vmem((2, rows // 2, width), bf16),
            vmem((6, rows // 2, width), bf16),
            vmem((2, 2, rows // 2, width), bf16),
            vmem((block, RING * ff), bf16),
            vmem((rows, width), bf16),
            pltpu.SemaphoreType.DMA((n_ids,)),
            pltpu.SemaphoreType.DMA((n_ids,)),
            pltpu.SemaphoreType.DMA((4 * layers,)),
        ]

        def kernel(*refs):
            ids = Ids()
            stack_kernel(layers, *refs, ids)
            assert ids.count <= n_ids, ids.count

        out = pl.pallas_call(
            kernel,
            out_shape=jax.ShapeDtypeStruct((rows, width), bf16),
            in_specs=[in_vmem, in_vmem, in_vmem, hbm, hbm, hbm, hbm],
            out_specs=in_vmem,
            scratch_shapes=scratch,
            compiler_params=pltpu.CompilerParams(collective_id=0, has_side_effects=True, vmem_limit_bytes=VMEM_LIMIT),
        )(x_local.reshape(rows, width), ln1_gain, ln2_gain, wqt, wo, w_up, w_down)
        return out.reshape(batch, rows, width)

    return jax.shard_map(layer_stack, mesh=mesh, in_specs=(P('dp', 'tp', None), P(), P(None, None, 'tp', None), P(None, 'tp', None, None), P(), P(None, None, 'tp'), P(None, 'tp', None)), out_specs=P('dp', 'tp', None), check_vma=False)
```

```python
import functools
import math

import jax
import jax.numpy as jnp
from jax import lax
from jax.experimental import pallas as pl
from jax.experimental.pallas import tpu as pltpu
from jax.sharding import PartitionSpec as P

LN_EPS = 1.0e-5
NEG_BIG = -1.0e30
MESH = pl.DeviceIdType.MESH
CORES = 2
VMEM_LIMIT = 67043328
OWN, LEFT, RIGHT, OPP = 0, 1, 2, 3
RING = 4


def layer_norm(resid_f32, ln_gain):
    row_mean = jnp.mean(resid_f32, axis=-1, keepdims=True)
    centered = resid_f32 - row_mean
    row_var = jnp.mean(centered * centered, axis=-1, keepdims=True)
    return (centered * lax.rsqrt(row_var + LN_EPS) * ln_gain).astype(jnp.bfloat16)


def dot(a, b, dims=((1,), (0,))):
    return lax.dot_general(a, b, (dims, ((), ())), preferred_element_type=jnp.float32)


class Ids:
    def __init__(self):
        self.count = 0

    def take(self, n):
        first = self.count
        self.count += n
        return first


def stack_kernel(layers, x_ref, g1_ref, g2_ref, wqt_ref, wo_ref, wu_ref, wd_ref, out_ref,
                 xg_a, xg_m, wq, wot, wu, wd, stage, qkv, keys, vals, ostage, score, osum, oall,
                 own, psend, precv, hop, comb, direct, hid, res,
                 send_sem, recv_sem, local_sem, ids):
    rows, width = res.shape
    half = rows // 2
    me = lax.axis_index("tp")
    part = lax.axis_index("dp") + 0 * me
    core = lax.rem(me, CORES)
    other = 1 - core
    xpos = lax.rem(lax.div(me, CORES), RING)
    ypos = lax.div(me, CORES * RING)

    def dev(y, x, c):
        return (lax.rem(y, RING) * RING + lax.rem(x, RING)) * CORES + c

    partner = dev(ypos, xpos, other)
    xdev = {LEFT: dev(ypos, xpos + 3, core), RIGHT: dev(ypos, xpos + 1, core), OPP: dev(ypos, xpos + 2, core)}
    ydev = {LEFT: dev(ypos + 3, xpos, core), RIGHT: dev(ypos + 1, xpos, core)}

    pending, pending_weights = {}, {}

    def send(k, src, dst, device, queue=pending):
        copy = pltpu.make_async_remote_copy(src_ref=src(), dst_ref=dst, send_sem=send_sem.at[k], recv_sem=recv_sem.at[k],
                                            device_id={"dp": part, "tp": device}, device_id_type=MESH)
        copy.start()
        if queue is not None:
            queue[k] = src

    def arrived(k, dst):
        pltpu.make_async_remote_copy(src_ref=dst, dst_ref=dst, send_sem=send_sem.at[k], recv_sem=recv_sem.at[k],
                                     device_id={"dp": part, "tp": partner}, device_id_type=MESH).wait_recv()

    def drain(queue=pending):
        for k, src in queue.items():
            pltpu.make_async_remote_copy(src_ref=src(), dst_ref=src(), send_sem=send_sem.at[k], recv_sem=recv_sem.at[k],
                                         device_id={"dp": part, "tp": partner}, device_id_type=MESH).wait_send()
        queue.clear()

    class Gather:
        def __init__(self, buf, ring):
            self.buf, self.ring, self.k = buf, ring, ids.take(12)
            self.a, self.b = pl.ds(0, half), pl.ds(half, half)

        def start(self):
            own_rows = self.buf.at[OWN, core]
            right, left = self.ring[RIGHT], self.ring[LEFT]
            send(self.k, lambda: own_rows.at[self.a], self.buf.at[LEFT, core, self.a], right)
            send(self.k + 1, lambda: own_rows.at[self.b], self.buf.at[RIGHT, core, self.b], left)
            send(self.k + 2, lambda: own_rows, self.buf.at[OWN, core], partner)
            send(self.k + 3, lambda: own_rows.at[self.b], self.buf.at[LEFT, core, self.b], right)
            send(self.k + 4, lambda: own_rows.at[self.a], self.buf.at[RIGHT, core, self.a], left)

        def relay(self):
            arrived(self.k, self.buf.at[LEFT, core, self.a])
            send(self.k + 5, lambda: self.buf.at[LEFT, core, self.a], self.buf.at[OPP, core, self.a], self.ring[RIGHT])
            arrived(self.k + 1, self.buf.at[RIGHT, core, self.b])
            send(self.k + 6, lambda: self.buf.at[RIGHT, core, self.b], self.buf.at[OPP, core, self.b], self.ring[LEFT])

        def near(self):
            arrived(self.k + 3, self.buf.at[LEFT, core, self.b])
            send(self.k + 7, lambda: self.buf.at[LEFT, core], self.buf.at[LEFT, core], partner)
            arrived(self.k + 4, self.buf.at[RIGHT, core, self.a])
            send(self.k + 8, lambda: self.buf.at[RIGHT, core], self.buf.at[RIGHT, core], partner)

        def far(self):
            arrived(self.k + 5, self.buf.at[OPP, core, self.a])
            arrived(self.k + 6, self.buf.at[OPP, core, self.b])
            send(self.k + 9, lambda: self.buf.at[OPP, core], self.buf.at[OPP, core], partner)

        def wait(self, slot):
            arrived(self.k + {OWN: 2, LEFT: 7, RIGHT: 8, OPP: 9}[slot], self.buf.at[slot, other])

    class Weights:
        def __init__(self, src, buf, ring):
            self.src, self.buf, self.ring = src, buf, ring
            self.k = ids.take(6)
            n = buf.shape[1] // 2
            self.a, self.b = pl.ds(0, n), pl.ds(n, n)

        def local(self, sem):
            copy = pltpu.make_async_copy(self.src, self.buf.at[OWN], local_sem.at[sem])
            copy.start()
            return copy

        def start(self):
            right, left = self.ring[RIGHT], self.ring[LEFT]
            send(self.k, lambda: self.src.at[self.a], self.buf.at[LEFT, self.a], right, pending_weights)
            send(self.k + 1, lambda: self.src.at[self.b], self.buf.at[RIGHT, self.b], left, pending_weights)

        def start_rest(self):
            right, left = self.ring[RIGHT], self.ring[LEFT]
            send(self.k + 2, lambda: self.src.at[self.b], self.buf.at[LEFT, self.b], right, pending_weights)
            send(self.k + 3, lambda: self.src.at[self.a], self.buf.at[RIGHT, self.a], left, pending_weights)

        def relay(self):
            arrived(self.k, self.buf.at[LEFT, self.a])
            send(self.k + 4, lambda: self.buf.at[LEFT, self.a], self.buf.at[OPP, self.a], self.ring[RIGHT], pending_weights)
            arrived(self.k + 1, self.buf.at[RIGHT, self.b])
            send(self.k + 5, lambda: self.buf.at[RIGHT, self.b], self.buf.at[OPP, self.b], self.ring[LEFT], pending_weights)

        def wait_near(self):
            arrived(self.k + 2, self.buf.at[LEFT, self.b])
            arrived(self.k + 3, self.buf.at[RIGHT, self.a])

        def wait_far(self):
            arrived(self.k + 4, self.buf.at[OPP, self.a])
            arrived(self.k + 5, self.buf.at[OPP, self.b])

    class Reduce:
        def __init__(self, ring):
            self.ring, self.k = ring, ids.take(10)
            self.a, self.b = pl.ds(0, half), pl.ds(half, half)

        def put(self, slot, cols, term):
            first, second = term[:rows], term[rows:]
            own[slot, :, cols] = jnp.where(core == 0, first, second)
            psend[slot, :, cols] = jnp.where(core == 0, second, first).astype(jnp.bfloat16)

        def give(self, slot):
            send(self.k + slot, lambda: psend.at[slot], precv.at[slot], partner)

        def pair(self, slot):
            arrived(self.k + slot, precv.at[slot])

        def term(self, slot, part):
            return own[slot, part, :] + precv[slot, part, :].astype(jnp.float32)

        def far(self):
            self.pair(OPP)
            comb[0] = self.term(OPP, self.a).astype(jnp.bfloat16)
            send(self.k + 4, lambda: comb.at[0], hop.at[0], self.ring[RIGHT])
            comb[1] = self.term(OPP, self.b).astype(jnp.bfloat16)
            send(self.k + 5, lambda: comb.at[1], hop.at[1], self.ring[LEFT])

        def near(self, slot):
            self.pair(slot)
            if slot == RIGHT:
                comb[2] = self.term(RIGHT, self.b).astype(jnp.bfloat16)
                send(self.k + 6, lambda: comb.at[2], direct.at[0, 1], self.ring[RIGHT])
            else:
                comb[3] = self.term(LEFT, self.a).astype(jnp.bfloat16)
                send(self.k + 7, lambda: comb.at[3], direct.at[1, 0], self.ring[LEFT])

        def relay(self):
            arrived(self.k + 4, hop.at[0])
            comb[4] = (self.term(RIGHT, self.a) + hop[0].astype(jnp.float32)).astype(jnp.bfloat16)
            send(self.k + 8, lambda: comb.at[4], direct.at[0, 0], self.ring[RIGHT])
            arrived(self.k + 5, hop.at[1])
            comb[5] = (self.term(LEFT, self.b) + hop[1].astype(jnp.float32)).astype(jnp.bfloat16)
            send(self.k + 9, lambda: comb.at[5], direct.at[1, 1], self.ring[LEFT])

        def finish(self):
            self.pair(OWN)
            arrived(self.k + 6, direct.at[0, 1])
            arrived(self.k + 7, direct.at[1, 0])
            arrived(self.k + 8, direct.at[0, 0])
            arrived(self.k + 9, direct.at[1, 1])
            for i, part in enumerate((self.a, self.b)):
                total = self.term(OWN, part) + direct[0, i].astype(jnp.float32) + direct[1, i].astype(jnp.float32)
                res[part, :] = (res[part, :].astype(jnp.float32) + total).astype(jnp.bfloat16)

    w_q = [Weights(wqt_ref.at[l], wq.at[l], xdev) for l in range(layers)]
    w_o = [Weights(wo_ref.at[l], wot.at[l], xdev) for l in range(layers)]
    w_u = [Weights(wu_ref.at[l], wu.at[l], ydev) for l in range(layers)]
    w_d = [Weights(wd_ref.at[l], wd.at[l], ydev) for l in range(layers)]
    everything = [w for l in range(layers) for w in (w_q[l], w_o[l], w_u[l], w_d[l])]
    copies = [w.local(i) for i, w in enumerate(everything)]

    barrier = pltpu.get_barrier_semaphore()
    peers = [partner, *xdev.values(), *ydev.values()]
    for peer in peers:
        pl.semaphore_signal(barrier, inc=1, device_id={"dp": part, "tp": peer}, device_id_type=MESH)
    res[...] = x_ref[...]
    pl.semaphore_wait(barrier, len(peers))

    head_dim = keys.shape[1]
    block = qkv.shape[2]
    column = RING * block

    def attention_front(l, gather):
        k = ids.take(3 * RING)
        order = (OWN, LEFT, RIGHT, OPP)

        def heads(s, slots):
            rows_in = xg_a[s].reshape(CORES * rows, width)
            n = len(slots)
            weights = wq[l, slots[0]:slots[0] + n].reshape(n * wq.shape[2], width)
            part = dot(weights, rows_in, ((1,), (1,))).astype(jnp.bfloat16).reshape(n, wq.shape[2], block)
            shift = {OWN: 0, LEFT: 3, RIGHT: 1, OPP: 2}[s]
            g = lax.rem(ypos + shift, RING) * RING + xpos
            for i, slot in enumerate(slots):
                if slot == OWN:
                    qkv[g] = part[i]
                else:
                    stage[s, slot - 1] = part[i]
                    send(k + 3 * s + slot - 1, lambda slot=slot: stage.at[s, slot - 1], qkv.at[g], xdev[slot])

        def receive():
            for s in order:
                shift = {OWN: 0, LEFT: 3, RIGHT: 1, OPP: 2}[s]
                for slot in (LEFT, RIGHT, OPP):
                    x_from = {LEFT: xpos + 1, RIGHT: xpos + 3, OPP: xpos + 2}[slot]
                    g = lax.rem(ypos + shift, RING) * RING + lax.rem(x_from, RING)
                    arrived(k + 3 * s + slot - 1, qkv.at[g])

        return heads, receive

    def prepare_keys():
        def body(g, carry):
            keys[pl.ds(pl.multiple_of(g * block, block), block), :] = (
                qkv[g, head_dim:2 * head_dim, :].astype(jnp.float32).T.astype(jnp.bfloat16))
            vals[g // RING, :, pl.ds(pl.multiple_of(lax.rem(g, RING) * block, block), block)] = qkv[g, 2 * head_dim:, :]
            return carry

        lax.fori_loop(0, RING * RING, body, 0)

    def attend(shift, i):
        y = lax.rem(ypos + shift, RING)
        queries = [(qkv[y * RING + x, :head_dim, :].astype(jnp.float32) * head_dim ** -0.5).astype(jnp.bfloat16)
                   for x in range(RING)]

        def step(chunk, state):
            k_all = keys[pl.ds(pl.multiple_of(chunk * column, column), column), :]
            v_all = vals[chunk]
            diagonal = state is None
            tops, new = [], []
            for x in range(RING):
                n = (x + 1) * block if diagonal else column
                s = dot(k_all[:n], queries[x])
                if diagonal:
                    key_pos = lax.broadcasted_iota(jnp.int32, (block, block), 0)
                    query_pos = lax.broadcasted_iota(jnp.int32, (block, block), 1)
                    last = jnp.where(query_pos >= key_pos, s[n - block:], NEG_BIG)
                    score[x, n - block:n, :] = last
                    top = jnp.max(last, axis=0, keepdims=True)
                    if x:
                        score[x, :n - block, :] = s[:n - block]
                        top = jnp.maximum(top, jnp.max(s[:n - block], axis=0, keepdims=True))
                else:
                    score[x] = s
                    top = jnp.max(s, axis=0, keepdims=True)
                tops.append(top)
            for x in range(RING):
                n = (x + 1) * block if diagonal else column
                top = tops[x] if diagonal else jnp.maximum(state[2 * x], tops[x])
                p = jnp.exp(score[x, :n, :] - top)
                total = jnp.sum(p, axis=0, keepdims=True)
                weighted = dot(v_all[:, :n], p.astype(jnp.bfloat16))
                if not diagonal:
                    scale = jnp.exp(state[2 * x] - top)
                    weighted = osum[x] * scale + weighted
                    total = state[2 * x + 1] * scale + total
                osum[x] = weighted
                new += [top, total]
            return tuple(new)

        state = lax.fori_loop(0, y, step, step(y, None))
        for x in range(RING):
            ostage[i, x] = (osum[x] / state[2 * x + 1]).astype(jnp.bfloat16)

    def exchange_o(i, k):
        oall[i, OWN] = ostage[i, xpos]
        for slot, x_to in ((LEFT, xpos + 1), (RIGHT, xpos + 3), (OPP, xpos + 2)):
            to = {LEFT: xdev[RIGHT], RIGHT: xdev[LEFT], OPP: xdev[OPP]}[slot]
            send(k + slot - 1, lambda x_to=x_to: ostage.at[i, lax.rem(x_to, RING)], oall.at[i, slot], to, None)

    def project(l, i, slot, k, reduce):
        for source in (LEFT, RIGHT, OPP):
            arrived(k + source - 1, oall.at[i, source])
        o_all = oall[i].reshape(RING * head_dim, block)
        tile = 1024

        def body(j, carry):
            cols = pl.ds(pl.multiple_of(j * tile, tile), tile)
            w_all = wot[l, :, :, cols].reshape(RING * head_dim, tile)
            reduce.put(slot, cols, dot(o_all, w_all, ((0,), (0,))))
            return carry

        lax.fori_loop(0, width // tile, body, 0)
        reduce.give(slot)

    def mlp_up(l, s, n=1):
        def up(j, carry):
            rows_in = xg_m[s:s + n].reshape(n * block, width)
            h = jax.nn.gelu(dot(rows_in, wu[l, j]), approximate=True).astype(jnp.bfloat16)
            hid[s:s + n, :, pl.ds(pl.multiple_of(j * wu.shape[3], wu.shape[3]), wu.shape[3])] = h.reshape(n, block, wu.shape[3])
            return carry

        lax.fori_loop(0, RING, up, 0)

    def mlp_down(l, s, reduce, n=1):
        tile = 512

        def down(j, carry):
            cols = pl.ds(pl.multiple_of(j * tile, tile), tile)
            w_all = wd[l, :, :, cols].reshape(hid.shape[2], tile)
            term = dot(hid[s:s + n].reshape(n * block, hid.shape[2]), w_all)
            for i in range(n):
                reduce.put(s + i, cols, term[i * block:(i + 1) * block])
            return carry

        lax.fori_loop(0, width // tile, down, 0)
        for i in range(n):
            reduce.give(s + i)

    def scoped(name, fn, *args):
        with jax.named_scope(name):
            return fn(*args)

    for l in range(layers):
        first, last = l == 0, l + 1 == layers
        scoped("drain", drain)
        gather = Gather(xg_a, ydev)
        xg_a[OWN, core] = layer_norm(res[...].astype(jnp.float32), g1_ref[l, :][None, :])
        gather.start()
        heads, receive = attention_front(l, gather)
        near = (OWN, LEFT, RIGHT)
        if first:
            w_q[l].start()
            w_q[l].start_rest()
            scoped("ag_relay", gather.relay)
            scoped("wq_relay", w_q[l].relay)
            scoped("ag_near", gather.near)
            w_u[l].start()
            w_u[l].start_rest()
            scoped("ag_far", gather.far)
            for i in range(2):
                copies[i].wait()
            scoped("wq_near", w_q[l].wait_near)
            for s in (*near, OPP):
                scoped("ag_wait", gather.wait, s)
                scoped("qkv", heads, s, near)
            scoped("wq_far", w_q[l].wait_far)
            for s in (*near, OPP):
                scoped("qkv", heads, s, (OPP,))
            w_o[l].start()
            w_o[l].start_rest()
        else:
            scoped("wq_near", w_q[l].wait_near)
            scoped("wq_far", w_q[l].wait_far)
            scoped("ag_wait", gather.wait, OWN)
            scoped("qkv", heads, OWN, (*near, OPP))
            scoped("ag_relay", gather.relay)
            scoped("ag_near", gather.near)
            w_o[l].start()
            w_o[l].start_rest()
            scoped("ag_wait", gather.wait, LEFT)
            scoped("qkv", heads, LEFT, (*near, OPP))
            scoped("ag_wait", gather.wait, RIGHT)
            scoped("qkv", heads, RIGHT, (*near, OPP))
            scoped("ag_far", gather.far)
            scoped("ag_wait", gather.wait, OPP)
            scoped("qkv", heads, OPP, (*near, OPP))
        scoped("wu_relay", w_u[l].relay)
        w_d[l].start()
        scoped("a2a_wait", receive)
        scoped("drain", drain)
        scoped("keys", prepare_keys)
        k_o = ids.take(3 * RING)
        reduce = Reduce(ydev)
        order = (OPP, LEFT, RIGHT, OWN)

        def finish_segment(i):
            project(l, i, order[i], k_o + 3 * i, reduce)

        def segment(i, carry):
            shift = lax.rem(2 + i + lax.div(i, 2) * (5 - 2 * i), RING)
            scoped("attend", attend, shift, i)
            exchange_o(i, k_o + 3 * i)

            @pl.when(i == 0)
            def _():
                scoped("wo_relay", w_o[l].relay)

            @pl.when(i == 1)
            def _():
                scoped("wo_near", w_o[l].wait_near)
                scoped("wo_far", w_o[l].wait_far)
                scoped("proj", finish_segment, 0)

            @pl.when(i == 2)
            def _():
                scoped("rs_far", reduce.far)
                scoped("proj", finish_segment, 1)

            return carry

        lax.fori_loop(0, RING, segment, 0)
        for i in range(RING):
            for slot, x_to in ((LEFT, xpos + 1), (RIGHT, xpos + 3), (OPP, xpos + 2)):
                pending[k_o + 3 * i + slot - 1] = lambda i=i, x_to=x_to: ostage.at[i, lax.rem(x_to, RING)]
        if not last:
            w_q[l + 1].start()
            w_q[l + 1].start_rest()
        scoped("proj", finish_segment, 2)
        scoped("rs_near", reduce.near, LEFT)
        scoped("proj", finish_segment, 3)
        scoped("rs_near", reduce.near, RIGHT)
        scoped("rs_relay", reduce.relay)
        w_d[l].start_rest()
        scoped("wd_relay", w_d[l].relay)
        if not last:
            scoped("wq_relay", w_q[l + 1].relay)
        scoped("rs_finish", reduce.finish)
        scoped("drain", drain)

        gather = Gather(xg_m, xdev)
        xg_m[OWN, core] = layer_norm(res[...].astype(jnp.float32), g2_ref[l, :][None, :])
        gather.start()
        if not last:
            w_u[l + 1].start()
            w_u[l + 1].start_rest()
        if first:
            for i in range(2, len(copies)):
                copies[i].wait()
        reduce = Reduce(xdev)
        scoped("wu_near", w_u[l].wait_near)
        scoped("wu_far", w_u[l].wait_far)
        scoped("ag_wait", gather.wait, OWN)
        scoped("up", mlp_up, l, OWN)
        scoped("ag_relay", gather.relay)
        scoped("ag_near", gather.near)
        scoped("ag_wait", gather.wait, LEFT)
        scoped("ag_wait", gather.wait, RIGHT)
        scoped("up", mlp_up, l, LEFT, 2)
        scoped("ag_far", gather.far)
        scoped("ag_wait", gather.wait, OPP)
        scoped("up", mlp_up, l, OPP)
        scoped("wd_near", w_d[l].wait_near)
        scoped("wd_far", w_d[l].wait_far)
        scoped("down", mlp_down, l, OPP, reduce)
        scoped("down", mlp_down, l, LEFT, reduce, 2)
        scoped("rs_far", reduce.far)
        scoped("down", mlp_down, l, OWN, reduce)
        scoped("rs_near", reduce.near, LEFT)
        scoped("rs_near", reduce.near, RIGHT)
        scoped("rs_relay", reduce.relay)
        scoped("rs_finish", reduce.finish)
    drain()
    drain(pending_weights)
    out_ref[...] = res[...]


def solution(mesh):
    def layer_stack(x_local, ln1_gain, w_qkv, w_out, ln2_gain, w_up, w_down):
        batch, rows, width = x_local.shape
        layers, _, _, three_e = w_qkv.shape
        head_dim = three_e // 3
        ff = w_up.shape[2]
        block = CORES * rows
        wqt = w_qkv.reshape(layers, width, three_e).transpose(0, 2, 1)
        wo = w_out.reshape(layers, head_dim, width)
        bf16, f32 = jnp.bfloat16, jnp.float32
        vmem = pltpu.VMEM
        n_ids = 200
        hbm = pl.BlockSpec(memory_space=pltpu.HBM)
        in_vmem = pl.BlockSpec(memory_space=pltpu.VMEM)
        scratch = [
            vmem((RING, CORES, rows, width), bf16),
            vmem((RING, CORES, rows, width), bf16),
            vmem((layers, RING, three_e, width), bf16),
            vmem((layers, RING, head_dim, width), bf16),
            vmem((layers, RING, width, ff), bf16),
            vmem((layers, RING, ff, width), bf16),
            vmem((RING, RING - 1, three_e, block), bf16),
            vmem((RING * RING, three_e, block), bf16),
            vmem((RING * RING * block, head_dim), bf16),
            vmem((RING, head_dim, RING * block), bf16),
            vmem((RING, RING, head_dim, block), bf16),
            vmem((RING, RING * block, block), f32),
            vmem((RING, head_dim, block), f32),
            vmem((RING, RING, head_dim, block), bf16),
            vmem((RING, rows, width), f32),
            vmem((RING, rows, width), bf16),
            vmem((RING, rows, width), bf16),
            vmem((2, rows // 2, width), bf16),
            vmem((6, rows // 2, width), bf16),
            vmem((2, 2, rows // 2, width), bf16),
            vmem((RING, block, RING * ff), bf16),
            vmem((rows, width), bf16),
            pltpu.SemaphoreType.DMA((n_ids,)),
            pltpu.SemaphoreType.DMA((n_ids,)),
            pltpu.SemaphoreType.DMA((4 * layers,)),
        ]

        def kernel(*refs):
            ids = Ids()
            stack_kernel(layers, *refs, ids)
            assert ids.count <= n_ids, ids.count

        out = pl.pallas_call(
            kernel,
            out_shape=jax.ShapeDtypeStruct((rows, width), bf16),
            in_specs=[in_vmem, in_vmem, in_vmem, hbm, hbm, hbm, hbm],
            out_specs=in_vmem,
            scratch_shapes=scratch,
            compiler_params=pltpu.CompilerParams(collective_id=0, has_side_effects=True, vmem_limit_bytes=VMEM_LIMIT),
        )(x_local.reshape(rows, width), ln1_gain, ln2_gain, wqt, wo, w_up, w_down)
        return out.reshape(batch, rows, width)

    return jax.shard_map(layer_stack, mesh=mesh, in_specs=(P('dp', 'tp', None), P(), P(None, None, 'tp', None), P(None, 'tp', None, None), P(), P(None, None, 'tp'), P(None, 'tp', None)), out_specs=P('dp', 'tp', None), check_vma=False)
```

```python
import functools
import math

import jax
import jax.numpy as jnp
from jax import lax
from jax.experimental import pallas as pl
from jax.experimental.pallas import tpu as pltpu
from jax.sharding import PartitionSpec as P

LN_EPS = 1.0e-5
NEG_BIG = -1.0e30
MESH = pl.DeviceIdType.MESH
CORES = 2
VMEM_LIMIT = 67043328
OWN, LEFT, RIGHT, OPP = 0, 1, 2, 3
RING = 4


def layer_norm(resid_f32, ln_gain):
    row_mean = jnp.mean(resid_f32, axis=-1, keepdims=True)
    centered = resid_f32 - row_mean
    row_var = jnp.mean(centered * centered, axis=-1, keepdims=True)
    return (centered * lax.rsqrt(row_var + LN_EPS) * ln_gain).astype(jnp.bfloat16)


def dot(a, b, dims=((1,), (0,))):
    return lax.dot_general(a, b, (dims, ((), ())), preferred_element_type=jnp.float32)


class Ids:
    def __init__(self):
        self.count = 0

    def take(self, n):
        first = self.count
        self.count += n
        return first


def stack_kernel(layers, x_ref, g1_ref, g2_ref, wqt_ref, wo_ref, wu_ref, wd_ref, out_ref,
                 xg_a, xg_m, wq, wot, wu, wd, stage, qkv, keys, vals, ostage, score, osum, oall,
                 own, psend, precv, hop, comb, direct, hid, res,
                 send_sem, recv_sem, local_sem, ids):
    rows, width = res.shape
    half = rows // 2
    me = lax.axis_index("tp")
    part = lax.axis_index("dp") + 0 * me
    core = lax.rem(me, CORES)
    other = 1 - core
    xpos = lax.rem(lax.div(me, CORES), RING)
    ypos = lax.div(me, CORES * RING)

    def dev(y, x, c):
        return (lax.rem(y, RING) * RING + lax.rem(x, RING)) * CORES + c

    partner = dev(ypos, xpos, other)
    xdev = {LEFT: dev(ypos, xpos + 3, core), RIGHT: dev(ypos, xpos + 1, core), OPP: dev(ypos, xpos + 2, core)}
    ydev = {LEFT: dev(ypos + 3, xpos, core), RIGHT: dev(ypos + 1, xpos, core)}

    pending, pending_weights, pending_early = {}, {}, {}

    def send(k, src, dst, device, queue=pending):
        copy = pltpu.make_async_remote_copy(src_ref=src(), dst_ref=dst, send_sem=send_sem.at[k], recv_sem=recv_sem.at[k],
                                            device_id={"dp": part, "tp": device}, device_id_type=MESH)
        copy.start()
        if queue is not None:
            queue[k] = src

    def arrived(k, dst):
        pltpu.make_async_remote_copy(src_ref=dst, dst_ref=dst, send_sem=send_sem.at[k], recv_sem=recv_sem.at[k],
                                     device_id={"dp": part, "tp": partner}, device_id_type=MESH).wait_recv()

    def drain(queue=pending):
        for k, src in queue.items():
            pltpu.make_async_remote_copy(src_ref=src(), dst_ref=src(), send_sem=send_sem.at[k], recv_sem=recv_sem.at[k],
                                         device_id={"dp": part, "tp": partner}, device_id_type=MESH).wait_send()
        queue.clear()

    class Gather:
        def __init__(self, buf, ring):
            self.buf, self.ring, self.k = buf, ring, ids.take(10)
            self.a, self.b = pl.ds(0, half), pl.ds(half, half)

        def start(self):
            own_rows = self.buf.at[OWN, core]
            right, left = self.ring[RIGHT], self.ring[LEFT]
            send(self.k, lambda: own_rows.at[self.a], self.buf.at[LEFT, core, self.a], right)
            send(self.k + 1, lambda: own_rows.at[self.b], self.buf.at[RIGHT, core, self.b], left)
            send(self.k + 2, lambda: own_rows, self.buf.at[OWN, core], partner)
            send(self.k + 3, lambda: own_rows.at[self.b], self.buf.at[LEFT, core, self.b], right)
            send(self.k + 4, lambda: own_rows.at[self.a], self.buf.at[RIGHT, core, self.a], left)

        def relay(self):
            arrived(self.k, self.buf.at[LEFT, core, self.a])
            send(self.k + 5, lambda: self.buf.at[LEFT, core, self.a], self.buf.at[OPP, core, self.a], self.ring[RIGHT])
            arrived(self.k + 1, self.buf.at[RIGHT, core, self.b])
            send(self.k + 6, lambda: self.buf.at[RIGHT, core, self.b], self.buf.at[OPP, core, self.b], self.ring[LEFT])

        def near(self):
            arrived(self.k + 3, self.buf.at[LEFT, core, self.b])
            send(self.k + 7, lambda: self.buf.at[LEFT, core], self.buf.at[LEFT, core], partner)
            arrived(self.k + 4, self.buf.at[RIGHT, core, self.a])
            send(self.k + 8, lambda: self.buf.at[RIGHT, core], self.buf.at[RIGHT, core], partner)

        def far(self):
            arrived(self.k + 5, self.buf.at[OPP, core, self.a])
            arrived(self.k + 6, self.buf.at[OPP, core, self.b])
            send(self.k + 9, lambda: self.buf.at[OPP, core], self.buf.at[OPP, core], partner)

        def wait(self, slot):
            arrived(self.k + {OWN: 2, LEFT: 7, RIGHT: 8, OPP: 9}[slot], self.buf.at[slot, other])

    class Weights:
        def __init__(self, src, buf, ring, k, queue):
            self.src, self.buf, self.ring, self.k, self.queue = src, buf, ring, k, queue
            n = buf.shape[1] // 2
            self.a, self.b = pl.ds(0, n), pl.ds(n, n)

        def local(self, sem):
            copy = pltpu.make_async_copy(self.src, self.buf.at[OWN], local_sem.at[sem])
            copy.start()
            return copy

        def start(self):
            right, left = self.ring[RIGHT], self.ring[LEFT]
            send(self.k, lambda: self.src.at[self.a], self.buf.at[LEFT, self.a], right, self.queue)
            send(self.k + 1, lambda: self.src.at[self.b], self.buf.at[RIGHT, self.b], left, self.queue)

        def start_rest(self):
            right, left = self.ring[RIGHT], self.ring[LEFT]
            send(self.k + 2, lambda: self.src.at[self.b], self.buf.at[LEFT, self.b], right, self.queue)
            send(self.k + 3, lambda: self.src.at[self.a], self.buf.at[RIGHT, self.a], left, self.queue)

        def relay(self):
            arrived(self.k, self.buf.at[LEFT, self.a])
            send(self.k + 4, lambda: self.buf.at[LEFT, self.a], self.buf.at[OPP, self.a], self.ring[RIGHT], self.queue)
            arrived(self.k + 1, self.buf.at[RIGHT, self.b])
            send(self.k + 5, lambda: self.buf.at[RIGHT, self.b], self.buf.at[OPP, self.b], self.ring[LEFT], self.queue)

        def wait_near(self):
            arrived(self.k + 2, self.buf.at[LEFT, self.b])
            arrived(self.k + 3, self.buf.at[RIGHT, self.a])

        def wait_far(self):
            arrived(self.k + 4, self.buf.at[OPP, self.a])
            arrived(self.k + 5, self.buf.at[OPP, self.b])

    class Reduce:
        def __init__(self, ring):
            self.ring, self.k = ring, ids.take(10)
            self.a, self.b = pl.ds(0, half), pl.ds(half, half)

        def put(self, slot, cols, term):
            first, second = term[:rows], term[rows:]
            own[slot, :, cols] = jnp.where(core == 0, first, second)
            psend[slot, :, cols] = jnp.where(core == 0, second, first).astype(jnp.bfloat16)

        def give(self, slot):
            send(self.k + slot, lambda: psend.at[slot], precv.at[slot], partner)

        def pair(self, slot):
            arrived(self.k + slot, precv.at[slot])

        def term(self, slot, part):
            return own[slot, part, :] + precv[slot, part, :].astype(jnp.float32)

        def far(self):
            self.pair(OPP)
            comb[0] = self.term(OPP, self.a).astype(jnp.bfloat16)
            send(self.k + 4, lambda: comb.at[0], hop.at[0], self.ring[RIGHT])
            comb[1] = self.term(OPP, self.b).astype(jnp.bfloat16)
            send(self.k + 5, lambda: comb.at[1], hop.at[1], self.ring[LEFT])

        def near(self, slot):
            self.pair(slot)
            if slot == RIGHT:
                comb[2] = self.term(RIGHT, self.b).astype(jnp.bfloat16)
                send(self.k + 6, lambda: comb.at[2], direct.at[0, 1], self.ring[RIGHT])
            else:
                comb[3] = self.term(LEFT, self.a).astype(jnp.bfloat16)
                send(self.k + 7, lambda: comb.at[3], direct.at[1, 0], self.ring[LEFT])

        def relay(self):
            arrived(self.k + 4, hop.at[0])
            comb[4] = (self.term(RIGHT, self.a) + hop[0].astype(jnp.float32)).astype(jnp.bfloat16)
            send(self.k + 8, lambda: comb.at[4], direct.at[0, 0], self.ring[RIGHT])
            arrived(self.k + 5, hop.at[1])
            comb[5] = (self.term(LEFT, self.b) + hop[1].astype(jnp.float32)).astype(jnp.bfloat16)
            send(self.k + 9, lambda: comb.at[5], direct.at[1, 1], self.ring[LEFT])

        def finish(self):
            self.pair(OWN)
            arrived(self.k + 6, direct.at[0, 1])
            arrived(self.k + 7, direct.at[1, 0])
            arrived(self.k + 8, direct.at[0, 0])
            arrived(self.k + 9, direct.at[1, 1])
            for i, part in enumerate((self.a, self.b)):
                total = self.term(OWN, part) + direct[0, i].astype(jnp.float32) + direct[1, i].astype(jnp.float32)
                res[part, :] = (res[part, :].astype(jnp.float32) + total).astype(jnp.bfloat16)

    k_q, k_w = ids.take(6), ids.take(6)
    w_q = [Weights(wqt_ref.at[l], wq.at[l], xdev, k_q, pending_early) for l in range(layers)]
    w_o = [Weights(wo_ref.at[l], wot.at[l], xdev, k_w, pending_early) for l in range(layers)]
    w_u = [Weights(wu_ref.at[l], wu.at[l], ydev, ids.take(6), pending_weights) for l in range(layers)]
    w_d = [Weights(wd_ref.at[l], wd.at[l], ydev, ids.take(6), pending_weights) for l in range(layers)]
    everything = [w for l in range(layers) for w in (w_q[l], w_o[l], w_u[l], w_d[l])]
    copies = [w.local(i) for i, w in enumerate(everything)]

    barrier = pltpu.get_barrier_semaphore()
    peers = [partner, *xdev.values(), *ydev.values()]
    for peer in peers:
        pl.semaphore_signal(barrier, inc=1, device_id={"dp": part, "tp": peer}, device_id_type=MESH)
    res[...] = x_ref[...]
    pl.semaphore_wait(barrier, len(peers))

    head_dim = keys.shape[1]
    block = qkv.shape[2]
    column = RING * block

    def attention_front(l, gather):
        k = ids.take(3 * RING)
        def heads(s, slots):
            rows_in = xg_a[s].reshape(CORES * rows, width)
            n = len(slots)
            weights = wq[l, slots[0]:slots[0] + n].reshape(n * wq.shape[2], width)
            part = dot(weights, rows_in, ((1,), (1,))).astype(jnp.bfloat16).reshape(n, wq.shape[2], block)
            shift = {OWN: 0, LEFT: 3, RIGHT: 1, OPP: 2}[s]
            g = lax.rem(ypos + shift, RING) * RING + xpos
            for i, slot in enumerate(slots):
                if slot == OWN:
                    qkv[g] = part[i]
                else:
                    stage[s, slot - 1] = part[i]
                    send(k + 3 * s + slot - 1, lambda slot=slot: stage.at[s, slot - 1], qkv.at[g], xdev[slot])

        def receive(s):
            shift = {OWN: 0, LEFT: 3, RIGHT: 1, OPP: 2}[s]
            y = lax.rem(ypos + shift, RING)
            for slot in (LEFT, RIGHT, OPP):
                x_from = {LEFT: xpos + 1, RIGHT: xpos + 3, OPP: xpos + 2}[slot]
                arrived(k + 3 * s + slot - 1, qkv.at[y * RING + lax.rem(x_from, RING)])
            return y

        return heads, receive

    def prepare_keys(y):
        def body(x, carry):
            g = y * RING + x
            keys[pl.ds(pl.multiple_of(g * block, block), block), :] = (
                qkv[g, head_dim:2 * head_dim, :].astype(jnp.float32).T.astype(jnp.bfloat16))
            vals[y, :, pl.ds(pl.multiple_of(x * block, block), block)] = qkv[g, 2 * head_dim:, :]
            return carry

        lax.fori_loop(0, RING, body, 0)

    def attend(shift, i):
        y = lax.rem(ypos + shift, RING)
        queries = [(qkv[y * RING + x, :head_dim, :].astype(jnp.float32) * head_dim ** -0.5).astype(jnp.bfloat16)
                   for x in range(RING)]

        def step(chunk, state):
            k_all = keys[pl.ds(pl.multiple_of(chunk * column, column), column), :]
            v_all = vals[chunk]
            diagonal = state is None
            tops, new = [], []
            for x in range(RING):
                n = (x + 1) * block if diagonal else column
                s = dot(k_all[:n], queries[x])
                if diagonal:
                    key_pos = lax.broadcasted_iota(jnp.int32, (block, block), 0)
                    query_pos = lax.broadcasted_iota(jnp.int32, (block, block), 1)
                    last = jnp.where(query_pos >= key_pos, s[n - block:], NEG_BIG)
                    score[x, n - block:n, :] = last
                    top = jnp.max(last, axis=0, keepdims=True)
                    if x:
                        score[x, :n - block, :] = s[:n - block]
                        top = jnp.maximum(top, jnp.max(s[:n - block], axis=0, keepdims=True))
                else:
                    score[x] = s
                    top = jnp.max(s, axis=0, keepdims=True)
                tops.append(top)
            for x in range(RING):
                n = (x + 1) * block if diagonal else column
                top = tops[x] if diagonal else jnp.maximum(state[2 * x], tops[x])
                p = jnp.exp(score[x, :n, :] - top)
                total = jnp.sum(p, axis=0, keepdims=True)
                weighted = dot(v_all[:, :n], p.astype(jnp.bfloat16))
                if not diagonal:
                    scale = jnp.exp(state[2 * x] - top)
                    weighted = osum[x] * scale + weighted
                    total = state[2 * x + 1] * scale + total
                osum[x] = weighted
                new += [top, total]
            return tuple(new)

        state = lax.fori_loop(0, y, step, step(y, None))
        for x in range(RING):
            ostage[i, x] = (osum[x] / state[2 * x + 1]).astype(jnp.bfloat16)

    def exchange_o(i, k):
        oall[i, OWN] = ostage[i, xpos]
        for slot, x_to in ((LEFT, xpos + 1), (RIGHT, xpos + 3), (OPP, xpos + 2)):
            to = {LEFT: xdev[RIGHT], RIGHT: xdev[LEFT], OPP: xdev[OPP]}[slot]
            send(k + slot - 1, lambda x_to=x_to: ostage.at[i, lax.rem(x_to, RING)], oall.at[i, slot], to, None)

    def project(l, i, slot, k, reduce):
        for source in (LEFT, RIGHT, OPP):
            arrived(k + source - 1, oall.at[i, source])
        o_all = oall[i].reshape(RING * head_dim, block)
        tile = 1024

        def body(j, carry):
            cols = pl.ds(pl.multiple_of(j * tile, tile), tile)
            w_all = wot[l, :, :, cols].reshape(RING * head_dim, tile)
            reduce.put(slot, cols, dot(o_all, w_all, ((0,), (0,))))
            return carry

        lax.fori_loop(0, width // tile, body, 0)
        reduce.give(slot)

    def mlp_up(l, s, n=1):
        def up(j, carry):
            rows_in = xg_m[s:s + n].reshape(n * block, width)
            h = jax.nn.gelu(dot(rows_in, wu[l, j]), approximate=True).astype(jnp.bfloat16)
            hid[s:s + n, :, pl.ds(pl.multiple_of(j * wu.shape[3], wu.shape[3]), wu.shape[3])] = h.reshape(n, block, wu.shape[3])
            return carry

        lax.fori_loop(0, RING, up, 0)

    def mlp_down(l, s, reduce, n=1):
        tile = 512

        def down(j, carry):
            cols = pl.ds(pl.multiple_of(j * tile, tile), tile)
            w_all = wd[l, :, :, cols].reshape(hid.shape[2], tile)
            term = dot(hid[s:s + n].reshape(n * block, hid.shape[2]), w_all)
            for i in range(n):
                reduce.put(s + i, cols, term[i * block:(i + 1) * block])
            return carry

        lax.fori_loop(0, width // tile, down, 0)
        for i in range(n):
            reduce.give(s + i)

    def scoped(name, fn, *args):
        with jax.named_scope(name):
            return fn(*args)

    first_id = ids.count
    for l in range(layers):
        ids.count = first_id
        first, last = l == 0, l + 1 == layers
        drain()
        gather = Gather(xg_a, ydev)
        xg_a[OWN, core] = layer_norm(res[...].astype(jnp.float32), g1_ref[l, :][None, :])
        gather.start()
        heads, receive = attention_front(l, gather)
        near = (OWN, LEFT, RIGHT)
        if first:
            w_q[l].start()
            w_q[l].start_rest()
            scoped("ag_relay", gather.relay)
            scoped("wq_relay", w_q[l].relay)
            scoped("ag_near", gather.near)
            w_u[l].start()
            w_u[l].start_rest()
            scoped("ag_far", gather.far)
            for i in range(2):
                copies[i].wait()
            scoped("wq_near", w_q[l].wait_near)
            for s in (*near, OPP):
                scoped("ag_wait", gather.wait, s)
                scoped("qkv", heads, s, near)
            scoped("wq_far", w_q[l].wait_far)
            for s in (*near, OPP):
                scoped("qkv", heads, s, (OPP,))
            w_o[l].start()
            w_o[l].start_rest()
        else:
            w_o[l].start()
            w_o[l].start_rest()
            scoped("wq_near", w_q[l].wait_near)
            scoped("wq_far", w_q[l].wait_far)
            scoped("ag_wait", gather.wait, OWN)
            scoped("qkv", heads, OWN, (*near, OPP))
            scoped("ag_relay", gather.relay)
            scoped("wo_relay", w_o[l].relay)
            scoped("ag_near", gather.near)
            scoped("ag_wait", gather.wait, LEFT)
            scoped("qkv", heads, LEFT, (*near, OPP))
            scoped("ag_wait", gather.wait, RIGHT)
            scoped("qkv", heads, RIGHT, (*near, OPP))
            scoped("ag_far", gather.far)
            scoped("ag_wait", gather.wait, OPP)
            scoped("qkv", heads, OPP, (*near, OPP))
        if first:
            scoped("wu_relay", w_u[l].relay)
        w_d[l].start()
        if not first:
            w_d[l].start_rest()
        for s in (*near, OPP):
            y = scoped("a2a_wait", receive, s)
            scoped("keys", prepare_keys, y)
        if first:
            scoped("wo_relay", w_o[l].relay)
        scoped("drain", drain)
        k_o = ids.take(3 * RING)
        reduce = Reduce(ydev)
        order = (OPP, LEFT, RIGHT, OWN)

        def finish_segment(i):
            project(l, i, order[i], k_o + 3 * i, reduce)

        def segment(i, carry):
            shift = lax.rem(2 + i + lax.div(i, 2) * (5 - 2 * i), RING)
            scoped("attend", attend, shift, i)
            exchange_o(i, k_o + 3 * i)

            @pl.when(i == 1)
            def _():
                scoped("wo_near", w_o[l].wait_near)
                scoped("wo_far", w_o[l].wait_far)
                scoped("proj", finish_segment, 0)

            @pl.when(i == 2)
            def _():
                scoped("rs_far", reduce.far)
                scoped("proj", finish_segment, 1)

            return carry

        lax.fori_loop(0, RING, segment, 0)
        for i in range(RING):
            for slot, x_to in ((LEFT, xpos + 1), (RIGHT, xpos + 3), (OPP, xpos + 2)):
                pending[k_o + 3 * i + slot - 1] = lambda i=i, x_to=x_to: ostage.at[i, lax.rem(x_to, RING)]
        if not last:
            drain(pending_early)
            w_q[l + 1].start()
            w_q[l + 1].start_rest()
        scoped("proj", finish_segment, 2)
        scoped("rs_near", reduce.near, LEFT)
        scoped("rs_near", reduce.near, RIGHT)
        scoped("proj", finish_segment, 3)
        scoped("rs_relay", reduce.relay)
        if first:
            w_d[l].start_rest()
        scoped("wd_relay", w_d[l].relay)
        scoped("rs_finish", reduce.finish)
        scoped("drain", drain)

        gather = Gather(xg_m, xdev)
        xg_m[OWN, core] = layer_norm(res[...].astype(jnp.float32), g2_ref[l, :][None, :])
        gather.start()
        if not last:
            w_u[l + 1].start()
            w_u[l + 1].start_rest()
        if first:
            for i in range(2, len(copies)):
                copies[i].wait()
        reduce = Reduce(xdev)
        scoped("wu_near", w_u[l].wait_near)
        scoped("wu_far", w_u[l].wait_far)
        scoped("ag_wait", gather.wait, OWN)
        scoped("up", mlp_up, l, OWN)
        scoped("ag_relay", gather.relay)
        scoped("ag_near", gather.near)
        if not first:
            scoped("wd_near", w_d[l].wait_near)
            scoped("wd_far", w_d[l].wait_far)
            scoped("down", mlp_down, l, OWN, reduce)
        scoped("ag_wait", gather.wait, LEFT)
        scoped("ag_wait", gather.wait, RIGHT)
        scoped("up", mlp_up, l, LEFT, 2)
        scoped("ag_far", gather.far)
        if not first:
            scoped("down", mlp_down, l, LEFT, reduce, 2)
        scoped("ag_wait", gather.wait, OPP)
        if not last:
            scoped("wq_relay", w_q[l + 1].relay)
        scoped("up", mlp_up, l, OPP)
        if first:
            scoped("wd_near", w_d[l].wait_near)
            scoped("wd_far", w_d[l].wait_far)
            scoped("down", mlp_down, l, OPP, reduce)
            scoped("down", mlp_down, l, LEFT, reduce, 2)
            scoped("rs_far", reduce.far)
            scoped("rs_near", reduce.near, LEFT)
            scoped("rs_near", reduce.near, RIGHT)
            scoped("down", mlp_down, l, OWN, reduce)
        else:
            scoped("rs_near", reduce.near, LEFT)
            scoped("rs_near", reduce.near, RIGHT)
            scoped("down", mlp_down, l, OPP, reduce)
            scoped("rs_far", reduce.far)
        scoped("rs_relay", reduce.relay)
        if not last:
            scoped("wu_relay", w_u[l + 1].relay)
        scoped("rs_finish", reduce.finish)
    drain()
    drain(pending_early)
    drain(pending_weights)
    out_ref[...] = res[...]


def solution(mesh):
    def layer_stack(x_local, ln1_gain, w_qkv, w_out, ln2_gain, w_up, w_down):
        batch, rows, width = x_local.shape
        layers, _, _, three_e = w_qkv.shape
        head_dim = three_e // 3
        ff = w_up.shape[2]
        block = CORES * rows
        wqt = w_qkv.reshape(layers, width, three_e).transpose(0, 2, 1)
        wo = w_out.reshape(layers, head_dim, width)
        bf16, f32 = jnp.bfloat16, jnp.float32
        vmem = pltpu.VMEM
        n_ids = 12 + 12 * layers + 64
        hbm = pl.BlockSpec(memory_space=pltpu.HBM)
        in_vmem = pl.BlockSpec(memory_space=pltpu.VMEM)
        scratch = [
            vmem((RING, CORES, rows, width), bf16),
            vmem((RING, CORES, rows, width), bf16),
            vmem((layers, RING, three_e, width), bf16),
            vmem((layers, RING, head_dim, width), bf16),
            vmem((layers, RING, width, ff), bf16),
            vmem((layers, RING, ff, width), bf16),
            vmem((RING, RING - 1, three_e, block), bf16),
            vmem((RING * RING, three_e, block), bf16),
            vmem((RING * RING * block, head_dim), bf16),
            vmem((RING, head_dim, RING * block), bf16),
            vmem((RING, RING, head_dim, block), bf16),
            vmem((RING, RING * block, block), f32),
            vmem((RING, head_dim, block), f32),
            vmem((RING, RING, head_dim, block), bf16),
            vmem((RING, rows, width), f32),
            vmem((RING, rows, width), bf16),
            vmem((RING, rows, width), bf16),
            vmem((2, rows // 2, width), bf16),
            vmem((6, rows // 2, width), bf16),
            vmem((2, 2, rows // 2, width), bf16),
            vmem((RING, block, RING * ff), bf16),
            vmem((rows, width), bf16),
            pltpu.SemaphoreType.DMA((n_ids,)),
            pltpu.SemaphoreType.DMA((n_ids,)),
            pltpu.SemaphoreType.DMA((4 * layers,)),
        ]

        def kernel(*refs):
            ids = Ids()
            stack_kernel(layers, *refs, ids)
            assert ids.count <= n_ids, ids.count

        out = pl.pallas_call(
            kernel,
            out_shape=jax.ShapeDtypeStruct((rows, width), bf16),
            in_specs=[in_vmem, in_vmem, in_vmem, hbm, hbm, hbm, hbm],
            out_specs=in_vmem,
            scratch_shapes=scratch,
            compiler_params=pltpu.CompilerParams(collective_id=0, has_side_effects=True, vmem_limit_bytes=VMEM_LIMIT),
        )(x_local.reshape(rows, width), ln1_gain, ln2_gain, wqt, wo, w_up, w_down)
        return out.reshape(batch, rows, width)

    return jax.shard_map(layer_stack, mesh=mesh, in_specs=(P('dp', 'tp', None), P(), P(None, None, 'tp', None), P(None, 'tp', None, None), P(), P(None, None, 'tp'), P(None, 'tp', None)), out_specs=P('dp', 'tp', None), check_vma=False)
```

```python
import functools
import math

import jax
import jax.numpy as jnp
from jax import lax
from jax.experimental import pallas as pl
from jax.experimental.pallas import tpu as pltpu
from jax.sharding import PartitionSpec as P

LN_EPS = 1.0e-5
NEG_BIG = -1.0e30
MESH = pl.DeviceIdType.MESH
CORES = 2
VMEM_LIMIT = 67043328
OWN, LEFT, RIGHT, OPP = 0, 1, 2, 3
RING = 4


def layer_norm(resid_f32, ln_gain):
    row_mean = jnp.mean(resid_f32, axis=-1, keepdims=True)
    centered = resid_f32 - row_mean
    row_var = jnp.mean(centered * centered, axis=-1, keepdims=True)
    return (centered * lax.rsqrt(row_var + LN_EPS) * ln_gain).astype(jnp.bfloat16)


def dot(a, b, dims=((1,), (0,))):
    return lax.dot_general(a, b, (dims, ((), ())), preferred_element_type=jnp.float32)


class Ids:
    def __init__(self):
        self.count = 0

    def take(self, n):
        first = self.count
        self.count += n
        return first


def stack_kernel(layers, x_ref, g1_ref, g2_ref, wqt_ref, wo_ref, wu_ref, wd_ref, out_ref,
                 xg_a, xg_m, wq, wot, wu, wd, stage, qkv, keys, vals, ostage, score, osum, oall,
                 own, psend, precv, hop, comb, direct, hid, res,
                 send_sem, recv_sem, local_sem, ids):
    rows, width = res.shape
    half = rows // 2
    me = lax.axis_index("tp")
    part = lax.axis_index("dp") + 0 * me
    core = lax.rem(me, CORES)
    other = 1 - core
    xpos = lax.rem(lax.div(me, CORES), RING)
    ypos = lax.div(me, CORES * RING)

    def dev(y, x, c):
        return (lax.rem(y, RING) * RING + lax.rem(x, RING)) * CORES + c

    partner = dev(ypos, xpos, other)
    xdev = {LEFT: dev(ypos, xpos + 3, core), RIGHT: dev(ypos, xpos + 1, core), OPP: dev(ypos, xpos + 2, core)}
    ydev = {LEFT: dev(ypos + 3, xpos, core), RIGHT: dev(ypos + 1, xpos, core)}

    pending, pending_weights, pending_early = {}, {}, {}

    def send(k, src, dst, device, queue=pending):
        copy = pltpu.make_async_remote_copy(src_ref=src(), dst_ref=dst, send_sem=send_sem.at[k], recv_sem=recv_sem.at[k],
                                            device_id={"dp": part, "tp": device}, device_id_type=MESH)
        copy.start()
        if queue is not None:
            queue[k] = src

    def arrived(k, dst):
        pltpu.make_async_remote_copy(src_ref=dst, dst_ref=dst, send_sem=send_sem.at[k], recv_sem=recv_sem.at[k],
                                     device_id={"dp": part, "tp": partner}, device_id_type=MESH).wait_recv()

    def drain(queue=pending):
        for k, src in queue.items():
            pltpu.make_async_remote_copy(src_ref=src(), dst_ref=src(), send_sem=send_sem.at[k], recv_sem=recv_sem.at[k],
                                         device_id={"dp": part, "tp": partner}, device_id_type=MESH).wait_send()
        queue.clear()

    class Gather:
        def __init__(self, buf, ring):
            self.buf, self.ring, self.k = buf, ring, ids.take(12)
            self.a, self.b = pl.ds(0, half), pl.ds(half, half)

        def start(self):
            own_rows = self.buf.at[OWN, core]
            right, left = self.ring[RIGHT], self.ring[LEFT]
            send(self.k, lambda: own_rows.at[self.a], self.buf.at[LEFT, core, self.a], right)
            send(self.k + 1, lambda: own_rows.at[self.b], self.buf.at[RIGHT, core, self.b], left)
            send(self.k + 2, lambda: own_rows, self.buf.at[OWN, core], partner)
            send(self.k + 3, lambda: own_rows.at[self.b], self.buf.at[LEFT, core, self.b], right)
            send(self.k + 4, lambda: own_rows.at[self.a], self.buf.at[RIGHT, core, self.a], left)

        def relay(self):
            arrived(self.k, self.buf.at[LEFT, core, self.a])
            send(self.k + 5, lambda: self.buf.at[LEFT, core, self.a], self.buf.at[OPP, core, self.a], self.ring[RIGHT])
            send(self.k + 7, lambda: self.buf.at[LEFT, core, self.a], self.buf.at[LEFT, core, self.a], partner)
            arrived(self.k + 1, self.buf.at[RIGHT, core, self.b])
            send(self.k + 6, lambda: self.buf.at[RIGHT, core, self.b], self.buf.at[OPP, core, self.b], self.ring[LEFT])
            send(self.k + 8, lambda: self.buf.at[RIGHT, core, self.b], self.buf.at[RIGHT, core, self.b], partner)

        def near(self):
            arrived(self.k + 3, self.buf.at[LEFT, core, self.b])
            send(self.k + 10, lambda: self.buf.at[LEFT, core, self.b], self.buf.at[LEFT, core, self.b], partner)
            arrived(self.k + 4, self.buf.at[RIGHT, core, self.a])
            send(self.k + 11, lambda: self.buf.at[RIGHT, core, self.a], self.buf.at[RIGHT, core, self.a], partner)

        def far(self):
            arrived(self.k + 5, self.buf.at[OPP, core, self.a])
            arrived(self.k + 6, self.buf.at[OPP, core, self.b])
            send(self.k + 9, lambda: self.buf.at[OPP, core], self.buf.at[OPP, core], partner)

        def wait(self, slot):
            if slot in (OWN, OPP):
                arrived(self.k + {OWN: 2, OPP: 9}[slot], self.buf.at[slot, other])
            else:
                first, second = {LEFT: (self.a, self.b), RIGHT: (self.b, self.a)}[slot]
                arrived(self.k + {LEFT: 7, RIGHT: 8}[slot], self.buf.at[slot, other, first])
                arrived(self.k + {LEFT: 10, RIGHT: 11}[slot], self.buf.at[slot, other, second])

    class Weights:
        def __init__(self, src, buf, ring, k, queue):
            self.src, self.buf, self.ring, self.k, self.queue = src, buf, ring, k, queue
            n = buf.shape[1] // 2
            self.a, self.b = pl.ds(0, n), pl.ds(n, n)

        def local(self, sem):
            copy = pltpu.make_async_copy(self.src, self.buf.at[OWN], local_sem.at[sem])
            copy.start()
            return copy

        def start(self):
            right, left = self.ring[RIGHT], self.ring[LEFT]
            send(self.k, lambda: self.src.at[self.a], self.buf.at[LEFT, self.a], right, self.queue)
            send(self.k + 1, lambda: self.src.at[self.b], self.buf.at[RIGHT, self.b], left, self.queue)

        def start_rest(self):
            right, left = self.ring[RIGHT], self.ring[LEFT]
            send(self.k + 2, lambda: self.src.at[self.b], self.buf.at[LEFT, self.b], right, self.queue)
            send(self.k + 3, lambda: self.src.at[self.a], self.buf.at[RIGHT, self.a], left, self.queue)

        def relay(self):
            arrived(self.k, self.buf.at[LEFT, self.a])
            send(self.k + 4, lambda: self.buf.at[LEFT, self.a], self.buf.at[OPP, self.a], self.ring[RIGHT], self.queue)
            arrived(self.k + 1, self.buf.at[RIGHT, self.b])
            send(self.k + 5, lambda: self.buf.at[RIGHT, self.b], self.buf.at[OPP, self.b], self.ring[LEFT], self.queue)

        def wait_near(self):
            arrived(self.k + 2, self.buf.at[LEFT, self.b])
            arrived(self.k + 3, self.buf.at[RIGHT, self.a])

        def wait_far(self):
            arrived(self.k + 4, self.buf.at[OPP, self.a])
            arrived(self.k + 5, self.buf.at[OPP, self.b])

    class Reduce:
        def __init__(self, ring):
            self.ring, self.k = ring, ids.take(10)
            self.a, self.b = pl.ds(0, half), pl.ds(half, half)

        def put(self, slot, cols, term):
            first, second = term[:rows], term[rows:]
            own[slot, :, cols] = jnp.where(core == 0, first, second)
            psend[slot, :, cols] = jnp.where(core == 0, second, first).astype(jnp.bfloat16)

        def give(self, slot):
            send(self.k + slot, lambda: psend.at[slot], precv.at[slot], partner)

        def pair(self, slot):
            arrived(self.k + slot, precv.at[slot])

        def term(self, slot, part):
            return own[slot, part, :] + precv[slot, part, :].astype(jnp.float32)

        def far(self):
            self.pair(OPP)
            comb[0] = self.term(OPP, self.a).astype(jnp.bfloat16)
            send(self.k + 4, lambda: comb.at[0], hop.at[0], self.ring[RIGHT])
            comb[1] = self.term(OPP, self.b).astype(jnp.bfloat16)
            send(self.k + 5, lambda: comb.at[1], hop.at[1], self.ring[LEFT])

        def near(self, slot):
            self.pair(slot)
            if slot == RIGHT:
                comb[2] = self.term(RIGHT, self.b).astype(jnp.bfloat16)
                send(self.k + 6, lambda: comb.at[2], direct.at[0, 1], self.ring[RIGHT])
            else:
                comb[3] = self.term(LEFT, self.a).astype(jnp.bfloat16)
                send(self.k + 7, lambda: comb.at[3], direct.at[1, 0], self.ring[LEFT])

        def relay(self):
            arrived(self.k + 4, hop.at[0])
            comb[4] = (self.term(RIGHT, self.a) + hop[0].astype(jnp.float32)).astype(jnp.bfloat16)
            send(self.k + 8, lambda: comb.at[4], direct.at[0, 0], self.ring[RIGHT])
            arrived(self.k + 5, hop.at[1])
            comb[5] = (self.term(LEFT, self.b) + hop[1].astype(jnp.float32)).astype(jnp.bfloat16)
            send(self.k + 9, lambda: comb.at[5], direct.at[1, 1], self.ring[LEFT])

        def finish(self):
            self.pair(OWN)
            arrived(self.k + 6, direct.at[0, 1])
            arrived(self.k + 7, direct.at[1, 0])
            arrived(self.k + 8, direct.at[0, 0])
            arrived(self.k + 9, direct.at[1, 1])
            for i, part in enumerate((self.a, self.b)):
                total = self.term(OWN, part) + direct[0, i].astype(jnp.float32) + direct[1, i].astype(jnp.float32)
                res[part, :] = (res[part, :].astype(jnp.float32) + total).astype(jnp.bfloat16)

    k_q, k_w = ids.take(6), ids.take(6)
    w_q = [Weights(wqt_ref.at[l], wq.at[l], xdev, k_q, pending_early) for l in range(layers)]
    w_o = [Weights(wo_ref.at[l], wot.at[l], xdev, k_w, pending_early) for l in range(layers)]
    w_u = [Weights(wu_ref.at[l], wu.at[l], ydev, ids.take(6), pending_weights) for l in range(layers)]
    w_d = [Weights(wd_ref.at[l], wd.at[l], ydev, ids.take(6), pending_weights) for l in range(layers)]
    everything = [w for l in range(layers) for w in (w_q[l], w_o[l], w_u[l], w_d[l])]
    copies = [w.local(i) for i, w in enumerate(everything)]

    barrier = pltpu.get_barrier_semaphore()
    peers = [partner, *xdev.values(), *ydev.values()]
    for peer in peers:
        pl.semaphore_signal(barrier, inc=1, device_id={"dp": part, "tp": peer}, device_id_type=MESH)
    res[...] = x_ref[...]
    pl.semaphore_wait(barrier, len(peers))

    head_dim = keys.shape[1]
    block = qkv.shape[2]
    column = RING * block

    def attention_front(l, gather):
        k = ids.take(3 * RING)
        def heads(s, slots):
            rows_in = xg_a[s].reshape(CORES * rows, width)
            n = len(slots)
            weights = wq[l, slots[0]:slots[0] + n].reshape(n * wq.shape[2], width)
            part = dot(weights, rows_in, ((1,), (1,))).astype(jnp.bfloat16).reshape(n, wq.shape[2], block)
            shift = {OWN: 0, LEFT: 3, RIGHT: 1, OPP: 2}[s]
            g = lax.rem(ypos + shift, RING) * RING + xpos
            for i, slot in enumerate(slots):
                if slot == OWN:
                    qkv[g] = part[i]
                else:
                    stage[s, slot - 1] = part[i]
                    send(k + 3 * s + slot - 1, lambda slot=slot: stage.at[s, slot - 1], qkv.at[g], xdev[slot])

        def receive(s):
            shift = {OWN: 0, LEFT: 3, RIGHT: 1, OPP: 2}[s]
            y = lax.rem(ypos + shift, RING)
            for slot in (LEFT, RIGHT, OPP):
                x_from = {LEFT: xpos + 1, RIGHT: xpos + 3, OPP: xpos + 2}[slot]
                arrived(k + 3 * s + slot - 1, qkv.at[y * RING + lax.rem(x_from, RING)])
            return y

        return heads, receive

    def prepare_keys(y):
        def body(x, carry):
            g = y * RING + x
            keys[pl.ds(pl.multiple_of(g * block, block), block), :] = (
                qkv[g, head_dim:2 * head_dim, :].astype(jnp.float32).T.astype(jnp.bfloat16))
            vals[y, :, pl.ds(pl.multiple_of(x * block, block), block)] = qkv[g, 2 * head_dim:, :]
            return carry

        lax.fori_loop(0, RING, body, 0)

    def attend(shift, i):
        y = lax.rem(ypos + shift, RING)
        queries = [(qkv[y * RING + x, :head_dim, :].astype(jnp.float32) * head_dim ** -0.5).astype(jnp.bfloat16)
                   for x in range(RING)]

        def step(chunk, state):
            k_all = keys[pl.ds(pl.multiple_of(chunk * column, column), column), :]
            v_all = vals[chunk]
            diagonal = state is None
            tops, new = [], []
            for x in range(RING):
                n = (x + 1) * block if diagonal else column
                s = dot(k_all[:n], queries[x])
                if diagonal:
                    key_pos = lax.broadcasted_iota(jnp.int32, (block, block), 0)
                    query_pos = lax.broadcasted_iota(jnp.int32, (block, block), 1)
                    last = jnp.where(query_pos >= key_pos, s[n - block:], NEG_BIG)
                    score[x, n - block:n, :] = last
                    top = jnp.max(last, axis=0, keepdims=True)
                    if x:
                        score[x, :n - block, :] = s[:n - block]
                        top = jnp.maximum(top, jnp.max(s[:n - block], axis=0, keepdims=True))
                else:
                    score[x] = s
                    top = jnp.max(s, axis=0, keepdims=True)
                tops.append(top)
            for x in range(RING):
                n = (x + 1) * block if diagonal else column
                top = tops[x] if diagonal else jnp.maximum(state[2 * x], tops[x])
                p = jnp.exp(score[x, :n, :] - top)
                total = jnp.sum(p, axis=0, keepdims=True)
                weighted = dot(v_all[:, :n], p.astype(jnp.bfloat16))
                if not diagonal:
                    scale = jnp.exp(state[2 * x] - top)
                    weighted = osum[x] * scale + weighted
                    total = state[2 * x + 1] * scale + total
                osum[x] = weighted
                new += [top, total]
            return tuple(new)

        state = lax.fori_loop(0, y, step, step(y, None))
        for x in range(RING):
            ostage[i, x] = (osum[x] / state[2 * x + 1]).astype(jnp.bfloat16)

    def exchange_o(i, k):
        oall[i, OWN] = ostage[i, xpos]
        for slot, x_to in ((LEFT, xpos + 1), (RIGHT, xpos + 3), (OPP, xpos + 2)):
            to = {LEFT: xdev[RIGHT], RIGHT: xdev[LEFT], OPP: xdev[OPP]}[slot]
            send(k + slot - 1, lambda x_to=x_to: ostage.at[i, lax.rem(x_to, RING)], oall.at[i, slot], to, None)

    def project(l, i, slot, k, reduce):
        for source in (LEFT, RIGHT, OPP):
            arrived(k + source - 1, oall.at[i, source])
        o_all = oall[i].reshape(RING * head_dim, block)
        tile = 1024

        def body(j, carry):
            cols = pl.ds(pl.multiple_of(j * tile, tile), tile)
            w_all = wot[l, :, :, cols].reshape(RING * head_dim, tile)
            reduce.put(slot, cols, dot(o_all, w_all, ((0,), (0,))))
            return carry

        lax.fori_loop(0, width // tile, body, 0)
        reduce.give(slot)

    def mlp_up(l, s, n=1):
        def up(j, carry):
            rows_in = xg_m[s:s + n].reshape(n * block, width)
            h = jax.nn.gelu(dot(rows_in, wu[l, j]), approximate=True).astype(jnp.bfloat16)
            hid[s:s + n, :, pl.ds(pl.multiple_of(j * wu.shape[3], wu.shape[3]), wu.shape[3])] = h.reshape(n, block, wu.shape[3])
            return carry

        lax.fori_loop(0, RING, up, 0, unroll=2)

    def mlp_down(l, s, reduce, n=1):
        tile = 512

        def down(j, carry):
            cols = pl.ds(pl.multiple_of(j * tile, tile), tile)
            w_all = wd[l, :, :, cols].reshape(hid.shape[2], tile)
            term = dot(hid[s:s + n].reshape(n * block, hid.shape[2]), w_all)
            for i in range(n):
                reduce.put(s + i, cols, term[i * block:(i + 1) * block])
            return carry

        lax.fori_loop(0, width // tile, down, 0, unroll=2)
        for i in range(n):
            reduce.give(s + i)

    def scoped(name, fn, *args):
        with jax.named_scope(name):
            return fn(*args)

    first_id = ids.count
    for l in range(layers):
        ids.count = first_id
        first, last = l == 0, l + 1 == layers
        drain()
        gather = Gather(xg_a, ydev)
        xg_a[OWN, core] = layer_norm(res[...].astype(jnp.float32), g1_ref[l, :][None, :])
        gather.start()
        heads, receive = attention_front(l, gather)
        near = (OWN, LEFT, RIGHT)
        if first:
            w_q[l].start()
            w_q[l].start_rest()
            scoped("ag_relay", gather.relay)
            scoped("wq_relay", w_q[l].relay)
            scoped("ag_near", gather.near)
            w_u[l].start()
            w_u[l].start_rest()
            scoped("ag_far", gather.far)
            for i in range(2):
                copies[i].wait()
            scoped("wq_near", w_q[l].wait_near)
            for s in (*near, OPP):
                scoped("ag_wait", gather.wait, s)
                scoped("qkv", heads, s, near)
            scoped("wq_far", w_q[l].wait_far)
            for s in (*near, OPP):
                scoped("qkv", heads, s, (OPP,))
            w_o[l].start()
            w_o[l].start_rest()
        else:
            w_o[l].start()
            w_o[l].start_rest()
            scoped("wq_near", w_q[l].wait_near)
            scoped("wq_far", w_q[l].wait_far)
            scoped("ag_wait", gather.wait, OWN)
            scoped("qkv", heads, OWN, (*near, OPP))
            scoped("ag_relay", gather.relay)
            scoped("wo_relay", w_o[l].relay)
            scoped("ag_near", gather.near)
            scoped("ag_wait", gather.wait, LEFT)
            scoped("qkv", heads, LEFT, (*near, OPP))
            scoped("ag_wait", gather.wait, RIGHT)
            scoped("qkv", heads, RIGHT, (*near, OPP))
            scoped("ag_far", gather.far)
            scoped("wu_relay", w_u[l].relay)
            scoped("ag_wait", gather.wait, OPP)
            scoped("qkv", heads, OPP, (*near, OPP))
        if first:
            scoped("wu_relay", w_u[l].relay)
        w_d[l].start()
        for s in (*near, OPP):
            y = scoped("a2a_wait", receive, s)
            scoped("keys", prepare_keys, y)
        scoped("drain", drain)
        k_o = ids.take(3 * RING)
        reduce = Reduce(ydev)
        order = (OPP, LEFT, RIGHT, OWN)

        def finish_segment(i):
            project(l, i, order[i], k_o + 3 * i, reduce)

        def segment(i, carry):
            shift = lax.rem(2 + i + lax.div(i, 2) * (5 - 2 * i), RING)
            scoped("attend", attend, shift, i)
            exchange_o(i, k_o + 3 * i)

            if first:
                @pl.when(i == 0)
                def _():
                    scoped("wo_relay", w_o[l].relay)

            @pl.when(i == 2)
            def _():
                scoped("wo_near", w_o[l].wait_near)
                scoped("wo_far", w_o[l].wait_far)
                scoped("proj", finish_segment, 0)
                scoped("rs_far", reduce.far)

            return carry

        lax.fori_loop(0, RING, segment, 0)
        for i in range(RING):
            for slot, x_to in ((LEFT, xpos + 1), (RIGHT, xpos + 3), (OPP, xpos + 2)):
                pending[k_o + 3 * i + slot - 1] = lambda i=i, x_to=x_to: ostage.at[i, lax.rem(x_to, RING)]
        if not last:
            drain(pending_early)
            w_q[l + 1].start()
            w_q[l + 1].start_rest()
        scoped("proj", finish_segment, 1)
        scoped("proj", finish_segment, 2)
        scoped("rs_near", reduce.near, LEFT)
        scoped("rs_near", reduce.near, RIGHT)
        scoped("proj", finish_segment, 3)
        scoped("rs_relay", reduce.relay)
        w_d[l].start_rest()
        scoped("wd_relay", w_d[l].relay)
        scoped("rs_finish", reduce.finish)
        scoped("drain", drain)

        gather = Gather(xg_m, xdev)
        xg_m[OWN, core] = layer_norm(res[...].astype(jnp.float32), g2_ref[l, :][None, :])
        gather.start()
        if not last:
            w_u[l + 1].start()
            w_u[l + 1].start_rest()
        if first:
            for i in range(2, len(copies)):
                copies[i].wait()
        reduce = Reduce(xdev)
        scoped("wu_near", w_u[l].wait_near)
        scoped("wu_far", w_u[l].wait_far)
        scoped("ag_wait", gather.wait, OWN)
        scoped("up", mlp_up, l, OWN)
        scoped("ag_relay", gather.relay)
        scoped("ag_near", gather.near)
        scoped("ag_wait", gather.wait, LEFT)
        scoped("ag_wait", gather.wait, RIGHT)
        scoped("up", mlp_up, l, LEFT, 2)
        scoped("ag_far", gather.far)
        if not first:
            scoped("wd_near", w_d[l].wait_near)
            scoped("wd_far", w_d[l].wait_far)
            scoped("down", mlp_down, l, LEFT, reduce, 2)
        scoped("ag_wait", gather.wait, OPP)
        if not last:
            scoped("wq_relay", w_q[l + 1].relay)
        scoped("up", mlp_up, l, OPP)
        if first:
            scoped("wd_near", w_d[l].wait_near)
            scoped("wd_far", w_d[l].wait_far)
            scoped("down", mlp_down, l, OPP, reduce)
            scoped("down", mlp_down, l, LEFT, reduce, 2)
            scoped("rs_far", reduce.far)
            scoped("rs_near", reduce.near, LEFT)
            scoped("rs_near", reduce.near, RIGHT)
            scoped("down", mlp_down, l, OWN, reduce)
        else:
            scoped("rs_near", reduce.near, LEFT)
            scoped("rs_near", reduce.near, RIGHT)
            scoped("down", mlp_down, l, OPP, reduce)
            scoped("rs_far", reduce.far)
            scoped("down", mlp_down, l, OWN, reduce)
        scoped("rs_relay", reduce.relay)
        scoped("rs_finish", reduce.finish)
    drain()
    drain(pending_early)
    drain(pending_weights)
    out_ref[...] = res[...]


def solution(mesh):
    def layer_stack(x_local, ln1_gain, w_qkv, w_out, ln2_gain, w_up, w_down):
        batch, rows, width = x_local.shape
        layers, _, _, three_e = w_qkv.shape
        head_dim = three_e // 3
        ff = w_up.shape[2]
        block = CORES * rows
        wqt = w_qkv.reshape(layers, width, three_e).transpose(0, 2, 1)
        wo = w_out.reshape(layers, head_dim, width)
        bf16, f32 = jnp.bfloat16, jnp.float32
        vmem = pltpu.VMEM
        n_ids = 12 + 12 * layers + 68
        hbm = pl.BlockSpec(memory_space=pltpu.HBM)
        in_vmem = pl.BlockSpec(memory_space=pltpu.VMEM)
        scratch = [
            vmem((RING, CORES, rows, width), bf16),
            vmem((RING, CORES, rows, width), bf16),
            vmem((layers, RING, three_e, width), bf16),
            vmem((layers, RING, head_dim, width), bf16),
            vmem((layers, RING, width, ff), bf16),
            vmem((layers, RING, ff, width), bf16),
            vmem((RING, RING - 1, three_e, block), bf16),
            vmem((RING * RING, three_e, block), bf16),
            vmem((RING * RING * block, head_dim), bf16),
            vmem((RING, head_dim, RING * block), bf16),
            vmem((RING, RING, head_dim, block), bf16),
            vmem((RING, RING * block, block), f32),
            vmem((RING, head_dim, block), f32),
            vmem((RING, RING, head_dim, block), bf16),
            vmem((RING, rows, width), f32),
            vmem((RING, rows, width), bf16),
            vmem((RING, rows, width), bf16),
            vmem((2, rows // 2, width), bf16),
            vmem((6, rows // 2, width), bf16),
            vmem((2, 2, rows // 2, width), bf16),
            vmem((RING, block, RING * ff), bf16),
            vmem((rows, width), bf16),
            pltpu.SemaphoreType.DMA((n_ids,)),
            pltpu.SemaphoreType.DMA((n_ids,)),
            pltpu.SemaphoreType.DMA((4 * layers,)),
        ]

        def kernel(*refs):
            ids = Ids()
            stack_kernel(layers, *refs, ids)
            assert ids.count <= n_ids, ids.count

        out = pl.pallas_call(
            kernel,
            out_shape=jax.ShapeDtypeStruct((rows, width), bf16),
            in_specs=[in_vmem, in_vmem, in_vmem, hbm, hbm, hbm, hbm],
            out_specs=in_vmem,
            scratch_shapes=scratch,
            compiler_params=pltpu.CompilerParams(collective_id=0, has_side_effects=True, vmem_limit_bytes=VMEM_LIMIT),
        )(x_local.reshape(rows, width), ln1_gain, ln2_gain, wqt, wo, w_up, w_down)
        return out.reshape(batch, rows, width)

    return jax.shard_map(layer_stack, mesh=mesh, in_specs=(P('dp', 'tp', None), P(), P(None, None, 'tp', None), P(None, 'tp', None, None), P(), P(None, None, 'tp'), P(None, 'tp', None)), out_specs=P('dp', 'tp', None), check_vma=False)
```

```python
import functools
import math

import jax
import jax.numpy as jnp
from jax import lax
from jax.experimental import pallas as pl
from jax.experimental.pallas import tpu as pltpu
from jax.sharding import PartitionSpec as P

LN_EPS = 1.0e-5
NEG_BIG = -1.0e30
MESH = pl.DeviceIdType.MESH
CORES = 2
VMEM_LIMIT = 67043328
OWN, LEFT, RIGHT, OPP = 0, 1, 2, 3
RING = 4


def layer_norm(resid_f32, ln_gain):
    row_mean = jnp.mean(resid_f32, axis=-1, keepdims=True)
    centered = resid_f32 - row_mean
    row_var = jnp.mean(centered * centered, axis=-1, keepdims=True)
    return (centered * lax.rsqrt(row_var + LN_EPS) * ln_gain).astype(jnp.bfloat16)


def dot(a, b, dims=((1,), (0,))):
    return lax.dot_general(a, b, (dims, ((), ())), preferred_element_type=jnp.float32)


class Ids:
    def __init__(self):
        self.count = 0

    def take(self, n):
        first = self.count
        self.count += n
        return first


def stack_kernel(layers, x_ref, g1_ref, g2_ref, wqt_ref, wo_ref, wu_ref, wd_ref, out_ref,
                 xg_a, xg_m, wq, wot, wu, wd, stage, qkv, keys, vals, ostage, score, osum, oall,
                 own, psend, precv, hop, comb, direct, hid, res,
                 send_sem, recv_sem, local_sem, ids):
    rows, width = res.shape
    half = rows // 2
    me = lax.axis_index("tp")
    part = lax.axis_index("dp") + 0 * me
    core = lax.rem(me, CORES)
    other = 1 - core
    xpos = lax.rem(lax.div(me, CORES), RING)
    ypos = lax.div(me, CORES * RING)

    def dev(y, x, c):
        return (lax.rem(y, RING) * RING + lax.rem(x, RING)) * CORES + c

    partner = dev(ypos, xpos, other)
    xdev = {LEFT: dev(ypos, xpos + 3, core), RIGHT: dev(ypos, xpos + 1, core), OPP: dev(ypos, xpos + 2, core)}
    ydev = {LEFT: dev(ypos + 3, xpos, core), RIGHT: dev(ypos + 1, xpos, core)}

    pending, pending_weights, pending_early = {}, {}, {}

    def send(k, src, dst, device, queue=pending):
        copy = pltpu.make_async_remote_copy(src_ref=src(), dst_ref=dst, send_sem=send_sem.at[k], recv_sem=recv_sem.at[k],
                                            device_id={"dp": part, "tp": device}, device_id_type=MESH)
        copy.start()
        if queue is not None:
            queue[k] = src

    def arrived(k, dst):
        pltpu.make_async_remote_copy(src_ref=dst, dst_ref=dst, send_sem=send_sem.at[k], recv_sem=recv_sem.at[k],
                                     device_id={"dp": part, "tp": partner}, device_id_type=MESH).wait_recv()

    def drain(queue=pending):
        for k, src in queue.items():
            pltpu.make_async_remote_copy(src_ref=src(), dst_ref=src(), send_sem=send_sem.at[k], recv_sem=recv_sem.at[k],
                                         device_id={"dp": part, "tp": partner}, device_id_type=MESH).wait_send()
        queue.clear()

    class Gather:
        def __init__(self, buf, ring):
            self.buf, self.ring, self.k = buf, ring, ids.take(12)
            self.a, self.b = pl.ds(0, half), pl.ds(half, half)

        def start(self):
            own_rows = self.buf.at[OWN, core]
            right, left = self.ring[RIGHT], self.ring[LEFT]
            send(self.k, lambda: own_rows.at[self.a], self.buf.at[LEFT, core, self.a], right)
            send(self.k + 1, lambda: own_rows.at[self.b], self.buf.at[RIGHT, core, self.b], left)
            send(self.k + 2, lambda: own_rows, self.buf.at[OWN, core], partner)
            send(self.k + 3, lambda: own_rows.at[self.b], self.buf.at[LEFT, core, self.b], right)
            send(self.k + 4, lambda: own_rows.at[self.a], self.buf.at[RIGHT, core, self.a], left)

        def relay(self):
            arrived(self.k, self.buf.at[LEFT, core, self.a])
            send(self.k + 5, lambda: self.buf.at[LEFT, core, self.a], self.buf.at[OPP, core, self.a], self.ring[RIGHT])
            send(self.k + 7, lambda: self.buf.at[LEFT, core, self.a], self.buf.at[LEFT, core, self.a], partner)
            arrived(self.k + 1, self.buf.at[RIGHT, core, self.b])
            send(self.k + 6, lambda: self.buf.at[RIGHT, core, self.b], self.buf.at[OPP, core, self.b], self.ring[LEFT])
            send(self.k + 8, lambda: self.buf.at[RIGHT, core, self.b], self.buf.at[RIGHT, core, self.b], partner)

        def near(self):
            arrived(self.k + 3, self.buf.at[LEFT, core, self.b])
            send(self.k + 10, lambda: self.buf.at[LEFT, core, self.b], self.buf.at[LEFT, core, self.b], partner)
            arrived(self.k + 4, self.buf.at[RIGHT, core, self.a])
            send(self.k + 11, lambda: self.buf.at[RIGHT, core, self.a], self.buf.at[RIGHT, core, self.a], partner)

        def far(self):
            arrived(self.k + 5, self.buf.at[OPP, core, self.a])
            arrived(self.k + 6, self.buf.at[OPP, core, self.b])
            send(self.k + 9, lambda: self.buf.at[OPP, core], self.buf.at[OPP, core], partner)

        def wait(self, slot):
            if slot in (OWN, OPP):
                arrived(self.k + {OWN: 2, OPP: 9}[slot], self.buf.at[slot, other])
            else:
                first, second = {LEFT: (self.a, self.b), RIGHT: (self.b, self.a)}[slot]
                arrived(self.k + {LEFT: 7, RIGHT: 8}[slot], self.buf.at[slot, other, first])
                arrived(self.k + {LEFT: 10, RIGHT: 11}[slot], self.buf.at[slot, other, second])

    class Weights:
        def __init__(self, src, buf, ring, k, queue):
            self.src, self.buf, self.ring, self.k, self.queue = src, buf, ring, k, queue
            n = buf.shape[1] // 2
            self.a, self.b = pl.ds(0, n), pl.ds(n, n)

        def local(self, sem):
            copy = pltpu.make_async_copy(self.src, self.buf.at[OWN], local_sem.at[sem])
            copy.start()
            return copy

        def start(self):
            right, left = self.ring[RIGHT], self.ring[LEFT]
            send(self.k, lambda: self.src.at[self.a], self.buf.at[LEFT, self.a], right, self.queue)
            send(self.k + 1, lambda: self.src.at[self.b], self.buf.at[RIGHT, self.b], left, self.queue)

        def start_rest(self):
            right, left = self.ring[RIGHT], self.ring[LEFT]
            send(self.k + 2, lambda: self.src.at[self.b], self.buf.at[LEFT, self.b], right, self.queue)
            send(self.k + 3, lambda: self.src.at[self.a], self.buf.at[RIGHT, self.a], left, self.queue)

        def relay(self):
            arrived(self.k, self.buf.at[LEFT, self.a])
            send(self.k + 4, lambda: self.buf.at[LEFT, self.a], self.buf.at[OPP, self.a], self.ring[RIGHT], self.queue)
            arrived(self.k + 1, self.buf.at[RIGHT, self.b])
            send(self.k + 5, lambda: self.buf.at[RIGHT, self.b], self.buf.at[OPP, self.b], self.ring[LEFT], self.queue)

        def wait_near(self):
            arrived(self.k + 2, self.buf.at[LEFT, self.b])
            arrived(self.k + 3, self.buf.at[RIGHT, self.a])

        def wait_far(self):
            arrived(self.k + 4, self.buf.at[OPP, self.a])
            arrived(self.k + 5, self.buf.at[OPP, self.b])

    class Reduce:
        def __init__(self, ring):
            self.ring, self.k = ring, ids.take(10)
            self.a, self.b = pl.ds(0, half), pl.ds(half, half)

        def put(self, slot, cols, term):
            first, second = term[:rows], term[rows:]
            own[slot, :, cols] = jnp.where(core == 0, first, second)
            psend[slot, :, cols] = jnp.where(core == 0, second, first).astype(jnp.bfloat16)

        def give(self, slot):
            send(self.k + slot, lambda: psend.at[slot], precv.at[slot], partner)

        def pair(self, slot):
            arrived(self.k + slot, precv.at[slot])

        def term(self, slot, part):
            return own[slot, part, :] + precv[slot, part, :].astype(jnp.float32)

        def far(self):
            self.pair(OPP)
            comb[0] = self.term(OPP, self.a).astype(jnp.bfloat16)
            send(self.k + 4, lambda: comb.at[0], hop.at[0], self.ring[RIGHT])
            comb[1] = self.term(OPP, self.b).astype(jnp.bfloat16)
            send(self.k + 5, lambda: comb.at[1], hop.at[1], self.ring[LEFT])

        def near(self, slot):
            self.pair(slot)
            if slot == RIGHT:
                comb[2] = self.term(RIGHT, self.b).astype(jnp.bfloat16)
                send(self.k + 6, lambda: comb.at[2], direct.at[0, 1], self.ring[RIGHT])
            else:
                comb[3] = self.term(LEFT, self.a).astype(jnp.bfloat16)
                send(self.k + 7, lambda: comb.at[3], direct.at[1, 0], self.ring[LEFT])

        def relay(self):
            arrived(self.k + 4, hop.at[0])
            comb[4] = (self.term(RIGHT, self.a) + hop[0].astype(jnp.float32)).astype(jnp.bfloat16)
            send(self.k + 8, lambda: comb.at[4], direct.at[0, 0], self.ring[RIGHT])
            arrived(self.k + 5, hop.at[1])
            comb[5] = (self.term(LEFT, self.b) + hop[1].astype(jnp.float32)).astype(jnp.bfloat16)
            send(self.k + 9, lambda: comb.at[5], direct.at[1, 1], self.ring[LEFT])

        def finish(self):
            self.pair(OWN)
            arrived(self.k + 6, direct.at[0, 1])
            arrived(self.k + 7, direct.at[1, 0])
            arrived(self.k + 8, direct.at[0, 0])
            arrived(self.k + 9, direct.at[1, 1])
            for i, part in enumerate((self.a, self.b)):
                total = self.term(OWN, part) + direct[0, i].astype(jnp.float32) + direct[1, i].astype(jnp.float32)
                res[part, :] = (res[part, :].astype(jnp.float32) + total).astype(jnp.bfloat16)

    k_q, k_w = ids.take(6), ids.take(6)
    w_q = [Weights(wqt_ref.at[l], wq.at[l], xdev, k_q, pending_early) for l in range(layers)]
    w_o = [Weights(wo_ref.at[l], wot.at[l], xdev, k_w, pending_early) for l in range(layers)]
    w_u = [Weights(wu_ref.at[l], wu.at[l], ydev, ids.take(6), pending_weights) for l in range(layers)]
    w_d = [Weights(wd_ref.at[l], wd.at[l], ydev, ids.take(6), pending_weights) for l in range(layers)]
    everything = [w for l in range(layers) for w in (w_q[l], w_o[l], w_u[l], w_d[l])]
    copies = [w.local(i) for i, w in enumerate(everything)]

    barrier = pltpu.get_barrier_semaphore()
    peers = [partner, *xdev.values(), *ydev.values()]
    for peer in peers:
        pl.semaphore_signal(barrier, inc=1, device_id={"dp": part, "tp": peer}, device_id_type=MESH)
    res[...] = x_ref[...]
    xg_a[OWN, core] = layer_norm(res[...].astype(jnp.float32), g1_ref[0, :][None, :])
    pl.semaphore_wait(barrier, len(peers))

    head_dim = keys.shape[1]
    block = qkv.shape[2]
    column = RING * block

    def attention_front(l, gather):
        k = ids.take(3 * RING)
        def heads(s, slots):
            rows_in = xg_a[s].reshape(CORES * rows, width)
            n = len(slots)
            weights = wq[l, slots[0]:slots[0] + n].reshape(n * wq.shape[2], width)
            part = dot(weights, rows_in, ((1,), (1,))).astype(jnp.bfloat16).reshape(n, wq.shape[2], block)
            shift = {OWN: 0, LEFT: 3, RIGHT: 1, OPP: 2}[s]
            g = lax.rem(ypos + shift, RING) * RING + xpos
            for i, slot in enumerate(slots):
                if slot == OWN:
                    qkv[g] = part[i]
                else:
                    stage[s, slot - 1] = part[i]
                    send(k + 3 * s + slot - 1, lambda slot=slot: stage.at[s, slot - 1], qkv.at[g], xdev[slot])

        def receive(s):
            shift = {OWN: 0, LEFT: 3, RIGHT: 1, OPP: 2}[s]
            y = lax.rem(ypos + shift, RING)
            for slot in (LEFT, RIGHT, OPP):
                x_from = {LEFT: xpos + 1, RIGHT: xpos + 3, OPP: xpos + 2}[slot]
                arrived(k + 3 * s + slot - 1, qkv.at[y * RING + lax.rem(x_from, RING)])
            return y

        return heads, receive

    def prepare_keys(y):
        def body(x, carry):
            g = y * RING + x
            keys[pl.ds(pl.multiple_of(g * block, block), block), :] = (
                qkv[g, head_dim:2 * head_dim, :].astype(jnp.float32).T.astype(jnp.bfloat16))
            vals[y, :, pl.ds(pl.multiple_of(x * block, block), block)] = qkv[g, 2 * head_dim:, :]
            return carry

        lax.fori_loop(0, RING, body, 0)

    def attend(shift, i):
        y = lax.rem(ypos + shift, RING)
        queries = [(qkv[y * RING + x, :head_dim, :].astype(jnp.float32) * head_dim ** -0.5).astype(jnp.bfloat16)
                   for x in range(RING)]

        def step(chunk, state):
            k_all = keys[pl.ds(pl.multiple_of(chunk * column, column), column), :]
            v_all = vals[chunk]
            diagonal = state is None
            tops, new = [], []
            for x in range(RING):
                n = (x + 1) * block if diagonal else column
                s = dot(k_all[:n], queries[x])
                if diagonal:
                    key_pos = lax.broadcasted_iota(jnp.int32, (block, block), 0)
                    query_pos = lax.broadcasted_iota(jnp.int32, (block, block), 1)
                    last = jnp.where(query_pos >= key_pos, s[n - block:], NEG_BIG)
                    score[x, n - block:n, :] = last
                    top = jnp.max(last, axis=0, keepdims=True)
                    if x:
                        score[x, :n - block, :] = s[:n - block]
                        top = jnp.maximum(top, jnp.max(s[:n - block], axis=0, keepdims=True))
                else:
                    score[x] = s
                    top = jnp.max(s, axis=0, keepdims=True)
                tops.append(top)
            for x in range(RING):
                n = (x + 1) * block if diagonal else column
                top = tops[x] if diagonal else jnp.maximum(state[2 * x], tops[x])
                p = jnp.exp(score[x, :n, :] - top)
                total = jnp.sum(p, axis=0, keepdims=True)
                weighted = dot(v_all[:, :n], p.astype(jnp.bfloat16))
                if not diagonal:
                    scale = jnp.exp(state[2 * x] - top)
                    weighted = osum[x] * scale + weighted
                    total = state[2 * x + 1] * scale + total
                osum[x] = weighted
                new += [top, total]
            return tuple(new)

        state = lax.fori_loop(0, y, step, step(y, None))
        for x in range(RING):
            ostage[i, x] = (osum[x] / state[2 * x + 1]).astype(jnp.bfloat16)

    def exchange_o(i, k):
        oall[i, OWN] = ostage[i, xpos]
        for slot, x_to in ((LEFT, xpos + 1), (RIGHT, xpos + 3), (OPP, xpos + 2)):
            to = {LEFT: xdev[RIGHT], RIGHT: xdev[LEFT], OPP: xdev[OPP]}[slot]
            send(k + slot - 1, lambda x_to=x_to: ostage.at[i, lax.rem(x_to, RING)], oall.at[i, slot], to, None)

    def project(l, i, slot, k, reduce):
        for source in (LEFT, RIGHT, OPP):
            arrived(k + source - 1, oall.at[i, source])
        o_all = oall[i].reshape(RING * head_dim, block)
        tile = 1024

        def body(j, carry):
            cols = pl.ds(pl.multiple_of(j * tile, tile), tile)
            w_all = wot[l, :, :, cols].reshape(RING * head_dim, tile)
            reduce.put(slot, cols, dot(o_all, w_all, ((0,), (0,))))
            return carry

        lax.fori_loop(0, width // tile, body, 0)
        reduce.give(slot)

    def mlp_up(l, s, n=1):
        def up(j, carry):
            rows_in = xg_m[s:s + n].reshape(n * block, width)
            h = jax.nn.gelu(dot(rows_in, wu[l, j]), approximate=True).astype(jnp.bfloat16)
            hid[s:s + n, :, pl.ds(pl.multiple_of(j * wu.shape[3], wu.shape[3]), wu.shape[3])] = h.reshape(n, block, wu.shape[3])
            return carry

        lax.fori_loop(0, RING, up, 0, unroll=2)

    def mlp_down(l, s, reduce, n=1):
        tile = 512

        def down(j, carry):
            cols = pl.ds(pl.multiple_of(j * tile, tile), tile)
            w_all = wd[l, :, :, cols].reshape(hid.shape[2], tile)
            term = dot(hid[s:s + n].reshape(n * block, hid.shape[2]), w_all)
            for i in range(n):
                reduce.put(s + i, cols, term[i * block:(i + 1) * block])
            return carry

        lax.fori_loop(0, width // tile, down, 0, unroll=2)
        for i in range(n):
            reduce.give(s + i)

    def scoped(name, fn, *args):
        with jax.named_scope(name):
            return fn(*args)

    first_id = ids.count
    for l in range(layers):
        ids.count = first_id
        first, last = l == 0, l + 1 == layers
        drain()
        gather = Gather(xg_a, ydev)
        if not first:
            xg_a[OWN, core] = layer_norm(res[...].astype(jnp.float32), g1_ref[l, :][None, :])
        gather.start()
        heads, receive = attention_front(l, gather)
        near = (OWN, LEFT, RIGHT)
        if first:
            w_q[l].start()
            w_q[l].start_rest()
            scoped("ag_relay", gather.relay)
            scoped("wq_relay", w_q[l].relay)
            scoped("ag_near", gather.near)
            w_u[l].start()
            w_u[l].start_rest()
            scoped("ag_far", gather.far)
            for i in range(2):
                copies[i].wait()
            scoped("wq_near", w_q[l].wait_near)
            for s in (*near, OPP):
                scoped("ag_wait", gather.wait, s)
                scoped("qkv", heads, s, near)
            scoped("wq_far", w_q[l].wait_far)
            for s in (*near, OPP):
                scoped("qkv", heads, s, (OPP,))
            w_o[l].start()
            w_o[l].start_rest()
        else:
            w_o[l].start()
            w_o[l].start_rest()
            scoped("ag_relay", gather.relay)
            scoped("wq_near", w_q[l].wait_near)
            scoped("wq_far", w_q[l].wait_far)
            scoped("ag_wait", gather.wait, OWN)
            scoped("qkv", heads, OWN, (*near, OPP))
            scoped("ag_near", gather.near)
            scoped("wo_relay", w_o[l].relay)
            scoped("ag_wait", gather.wait, LEFT)
            scoped("qkv", heads, LEFT, (*near, OPP))
            scoped("ag_wait", gather.wait, RIGHT)
            scoped("qkv", heads, RIGHT, (*near, OPP))
            scoped("ag_far", gather.far)
            scoped("wu_relay", w_u[l].relay)
            scoped("ag_wait", gather.wait, OPP)
            scoped("qkv", heads, OPP, (*near, OPP))
        if first:
            scoped("wu_relay", w_u[l].relay)
        w_d[l].start()
        for s in (*near, OPP):
            y = scoped("a2a_wait", receive, s)
            scoped("keys", prepare_keys, y)
        scoped("drain", drain)
        k_o = ids.take(3 * RING)
        reduce = Reduce(ydev)
        order = (OPP, LEFT, RIGHT, OWN)

        def finish_segment(i):
            project(l, i, order[i], k_o + 3 * i, reduce)

        def segment(i, carry):
            shift = lax.rem(2 + i + lax.div(i, 2) * (5 - 2 * i), RING)
            scoped("attend", attend, shift, i)
            exchange_o(i, k_o + 3 * i)

            if first:
                @pl.when(i == 0)
                def _():
                    scoped("wo_relay", w_o[l].relay)

            @pl.when(i == 2)
            def _():
                scoped("wo_near", w_o[l].wait_near)
                scoped("wo_far", w_o[l].wait_far)
                scoped("proj", finish_segment, 0)
                scoped("rs_far", reduce.far)

            return carry

        lax.fori_loop(0, RING, segment, 0)
        for i in range(RING):
            for slot, x_to in ((LEFT, xpos + 1), (RIGHT, xpos + 3), (OPP, xpos + 2)):
                pending[k_o + 3 * i + slot - 1] = lambda i=i, x_to=x_to: ostage.at[i, lax.rem(x_to, RING)]
        if not last:
            drain(pending_early)
            w_q[l + 1].start()
            w_q[l + 1].start_rest()
        scoped("proj", finish_segment, 1)
        scoped("proj", finish_segment, 2)
        scoped("rs_near", reduce.near, LEFT)
        scoped("rs_near", reduce.near, RIGHT)
        scoped("proj", finish_segment, 3)
        scoped("rs_relay", reduce.relay)
        w_d[l].start_rest()
        scoped("wd_relay", w_d[l].relay)
        scoped("rs_finish", reduce.finish)
        scoped("drain", drain)

        gather = Gather(xg_m, xdev)
        xg_m[OWN, core] = layer_norm(res[...].astype(jnp.float32), g2_ref[l, :][None, :])
        gather.start()
        if not last:
            w_u[l + 1].start()
            w_u[l + 1].start_rest()
        if first:
            for i in range(2, len(copies)):
                copies[i].wait()
        reduce = Reduce(xdev)
        scoped("wu_near", w_u[l].wait_near)
        scoped("wu_far", w_u[l].wait_far)
        scoped("ag_wait", gather.wait, OWN)
        scoped("up", mlp_up, l, OWN)
        scoped("ag_relay", gather.relay)
        scoped("ag_near", gather.near)
        scoped("ag_wait", gather.wait, LEFT)
        scoped("ag_wait", gather.wait, RIGHT)
        scoped("up", mlp_up, l, LEFT, 2)
        scoped("ag_far", gather.far)
        if not first:
            scoped("wd_near", w_d[l].wait_near)
            scoped("wd_far", w_d[l].wait_far)
            scoped("down", mlp_down, l, LEFT, reduce, 2)
        scoped("ag_wait", gather.wait, OPP)
        scoped("up", mlp_up, l, OPP)
        if first:
            scoped("wd_near", w_d[l].wait_near)
            scoped("wd_far", w_d[l].wait_far)
            scoped("down", mlp_down, l, OPP, reduce)
            scoped("down", mlp_down, l, LEFT, reduce, 2)
            scoped("rs_far", reduce.far)
            scoped("rs_near", reduce.near, LEFT)
            scoped("rs_near", reduce.near, RIGHT)
            scoped("down", mlp_down, l, OWN, reduce)
        else:
            scoped("rs_near", reduce.near, LEFT)
            scoped("rs_near", reduce.near, RIGHT)
            scoped("down", mlp_down, l, OPP, reduce)
            scoped("rs_far", reduce.far)
            scoped("down", mlp_down, l, OWN, reduce)
        scoped("rs_relay", reduce.relay)
        if not last:
            scoped("wq_relay", w_q[l + 1].relay)
        scoped("rs_finish", reduce.finish)
    drain()
    drain(pending_early)
    drain(pending_weights)
    out_ref[...] = res[...]


def solution(mesh):
    def layer_stack(x_local, ln1_gain, w_qkv, w_out, ln2_gain, w_up, w_down):
        batch, rows, width = x_local.shape
        layers, _, _, three_e = w_qkv.shape
        head_dim = three_e // 3
        ff = w_up.shape[2]
        block = CORES * rows
        wqt = w_qkv.reshape(layers, width, three_e).transpose(0, 2, 1)
        wo = w_out.reshape(layers, head_dim, width)
        bf16, f32 = jnp.bfloat16, jnp.float32
        vmem = pltpu.VMEM
        n_ids = 12 + 12 * layers + 68
        hbm = pl.BlockSpec(memory_space=pltpu.HBM)
        in_vmem = pl.BlockSpec(memory_space=pltpu.VMEM)
        scratch = [
            vmem((RING, CORES, rows, width), bf16),
            vmem((RING, CORES, rows, width), bf16),
            vmem((layers, RING, three_e, width), bf16),
            vmem((layers, RING, head_dim, width), bf16),
            vmem((layers, RING, width, ff), bf16),
            vmem((layers, RING, ff, width), bf16),
            vmem((RING, RING - 1, three_e, block), bf16),
            vmem((RING * RING, three_e, block), bf16),
            vmem((RING * RING * block, head_dim), bf16),
            vmem((RING, head_dim, RING * block), bf16),
            vmem((RING, RING, head_dim, block), bf16),
            vmem((RING, RING * block, block), f32),
            vmem((RING, head_dim, block), f32),
            vmem((RING, RING, head_dim, block), bf16),
            vmem((RING, rows, width), f32),
            vmem((RING, rows, width), bf16),
            vmem((RING, rows, width), bf16),
            vmem((2, rows // 2, width), bf16),
            vmem((6, rows // 2, width), bf16),
            vmem((2, 2, rows // 2, width), bf16),
            vmem((RING, block, RING * ff), bf16),
            vmem((rows, width), bf16),
            pltpu.SemaphoreType.DMA((n_ids,)),
            pltpu.SemaphoreType.DMA((n_ids,)),
            pltpu.SemaphoreType.DMA((4 * layers,)),
        ]

        def kernel(*refs):
            ids = Ids()
            stack_kernel(layers, *refs, ids)
            assert ids.count <= n_ids, ids.count

        out = pl.pallas_call(
            kernel,
            out_shape=jax.ShapeDtypeStruct((rows, width), bf16),
            in_specs=[in_vmem, in_vmem, in_vmem, hbm, hbm, hbm, hbm],
            out_specs=in_vmem,
            scratch_shapes=scratch,
            compiler_params=pltpu.CompilerParams(collective_id=0, has_side_effects=True, vmem_limit_bytes=VMEM_LIMIT),
        )(x_local.reshape(rows, width), ln1_gain, ln2_gain, wqt, wo, w_up, w_down)
        return out.reshape(batch, rows, width)

    return jax.shard_map(layer_stack, mesh=mesh, in_specs=(P('dp', 'tp', None), P(), P(None, None, 'tp', None), P(None, 'tp', None, None), P(), P(None, None, 'tp'), P(None, 'tp', None)), out_specs=P('dp', 'tp', None), check_vma=False)
```
